8 devices in a mesh: dp: 2 (over z, y), sp: 4 (over x, core).
Axes of the slice: x: 2, y: 2, z: 1, core: 2. Of those that a mesh axis runs over, the one named last changes fastest.
Arguments:
- hidden: bfloat16 [512, 6144], P(('dp', 'sp')), parts along dimension 0
- w_q: bfloat16 [6144, 6144], replicated
- w_k: bfloat16 [6144, 1024], replicated
- w_v: bfloat16 [6144, 1024], replicated
- w_o: bfloat16 [6144, 6144], replicated
- expert_ids: int32 [512, 2], P(('dp', 'sp')), parts along dimension 0
- router_probs: float32 [512, 8], P(('dp', 'sp')), parts along dimension 0
Outputs:
- output 1: bfloat16 [512, 6144], P(('dp', 'sp')), parts along dimension 0
- output 2: bfloat16 [16, 256, 6144], P(('dp', 'sp')), parts along dimension 0
There are 2 independent parts. The reference program is written for one: setup_inputs(seed, part) draws one part's arguments, and reference() takes and returns one part's arrays. A program takes and returns all parts, laid end to end along the dimension named above; an argument that names none is the same for every part.
All inputs are finite; a program needn't handle non-finite values.
Results may differ from the reference program's by a relative error of at most 0.00851991.
Values are sent between devices in bfloat16 or wider.
A program may use at most 1 GiB of HBM per device.

```python
import math
import jax
import jax.numpy as jnp
from jax import lax

D = 6144
HEADS = 48
KV_HEADS = 8
HEAD = 128
EXPERTS = 8
TOKENS_DEV = 64
GROUP = 4

SEQ = TOKENS_DEV * GROUP
Q_PER_KV = HEADS // KV_HEADS
Q_WIDTH = HEADS * HEAD
KV_WIDTH = KV_HEADS * HEAD
SCORE_SCALE = 1.0 / math.sqrt(HEAD)


def draw_routes(route_key):
    key_first, key_second, key_pick, key_cold, key_order = jax.random.split(route_key, 5)
    hot_first = jax.random.randint(key_first, (), 0, EXPERTS)
    hot_second = (hot_first + 1 + jax.random.randint(key_second, (), 0, EXPERTS - 1)) % EXPERTS
    pick_hot = jax.random.randint(key_pick, (SEQ,), 0, 2)
    cold_ids = (hot_first + 1 + jax.random.randint(key_cold, (SEQ,), 0, EXPERTS - 1)) % EXPERTS
    other_ids = jnp.where(pick_hot == 1, hot_second, cold_ids)
    first_ids = jnp.full((SEQ,), hot_first)
    swap_bits = jax.random.randint(key_order, (SEQ,), 0, 2)
    col_zero = jnp.where(swap_bits == 1, other_ids, first_ids)
    col_one = jnp.where(swap_bits == 1, first_ids, other_ids)
    return jnp.stack([col_zero, col_one], axis=1).astype(jnp.int32)


def setup_inputs(seed: int = 0, part: int = 0) -> dict:
    base_key = jax.random.key(seed)
    part_key = jax.random.fold_in(base_key, part)
    weight_keys = jax.random.split(base_key, 4)
    part_keys = jax.random.split(part_key, 3)
    q_gain = math.sqrt(0.5 * math.log(SEQ))
    o_gain = 0.5 * SEQ ** 0.25
    hidden = jax.random.normal(part_keys[0], (SEQ, D), jnp.float32).astype(jnp.bfloat16)
    w_q = (jax.random.normal(weight_keys[0], (D, Q_WIDTH), jnp.float32) * (q_gain / math.sqrt(D))).astype(jnp.bfloat16)
    w_k = (jax.random.normal(weight_keys[1], (D, KV_WIDTH), jnp.float32) / math.sqrt(D)).astype(jnp.bfloat16)
    w_v = (jax.random.normal(weight_keys[2], (D, KV_WIDTH), jnp.float32) / math.sqrt(D)).astype(jnp.bfloat16)
    w_o = (jax.random.normal(weight_keys[3], (Q_WIDTH, D), jnp.float32) * (o_gain / math.sqrt(Q_WIDTH))).astype(jnp.bfloat16)
    expert_ids = draw_routes(part_keys[1])
    router_probs = jax.nn.softmax(1.5 * jax.random.normal(part_keys[2], (SEQ, EXPERTS), jnp.float32), axis=1)
    return {'hidden': hidden, 'w_q': w_q, 'w_k': w_k, 'w_v': w_v, 'w_o': w_o, 'expert_ids': expert_ids, 'router_probs': router_probs}


def reference(hidden, w_q, w_k, w_v, w_o, expert_ids, router_probs):
    q_all = jnp.dot(hidden, w_q, preferred_element_type=jnp.float32).astype(jnp.bfloat16)
    k_all = jnp.dot(hidden, w_k, preferred_element_type=jnp.float32).astype(jnp.bfloat16)
    v_all = jnp.dot(hidden, w_v, preferred_element_type=jnp.float32).astype(jnp.bfloat16)
    q_groups = q_all.reshape(SEQ, KV_HEADS, Q_PER_KV, HEAD).transpose(1, 0, 2, 3)
    k_groups = k_all.reshape(SEQ, KV_HEADS, HEAD).transpose(1, 0, 2)
    v_groups = v_all.reshape(SEQ, KV_HEADS, HEAD).transpose(1, 0, 2)
    positions = jnp.arange(SEQ)
    causal = positions[:, None] >= positions[None, :]

    def one_group(group_in):
        q_grp, k_grp, v_grp = group_in
        scores = jnp.einsum('qmd,kd->mqk', q_grp.astype(jnp.float32), k_grp.astype(jnp.float32)) * SCORE_SCALE
        scores = jnp.where(causal[None, :, :], scores, -1e30)
        weights = jax.nn.softmax(scores, axis=-1).astype(jnp.bfloat16)
        out_grp = jnp.einsum('mqk,kd->qmd', weights.astype(jnp.float32), v_grp.astype(jnp.float32))
        return out_grp.astype(jnp.bfloat16)

    attn_out = lax.map(one_group, (q_groups, k_groups, v_groups))
    attn_out = attn_out.transpose(1, 0, 2, 3).reshape(SEQ, Q_WIDTH)
    out_proj = jnp.dot(attn_out, w_o, preferred_element_type=jnp.float32)
    hidden_out = (hidden.astype(jnp.float32) + out_proj).astype(jnp.bfloat16)
    picked = jnp.take_along_axis(router_probs, expert_ids, axis=1)
    gate_w = picked / jnp.sum(picked, axis=1, keepdims=True)
    gated = (gate_w[:, :, None] * hidden_out.astype(jnp.float32)[:, None, :]).astype(jnp.bfloat16)
    ids_blk = expert_ids.reshape(GROUP, TOKENS_DEV, 2)
    token_hits = jnp.sum((ids_blk[:, :, :, None] == jnp.arange(EXPERTS)).astype(jnp.int32), axis=2)
    earlier = jnp.cumsum(token_hits, axis=1) - token_hits
    slot_rank = jnp.take_along_axis(earlier, ids_blk, axis=2)
    dest_rows = jnp.arange(GROUP)[:, None, None] * TOKENS_DEV + slot_rank
    buffer = jnp.zeros((EXPERTS, GROUP * TOKENS_DEV, D), jnp.bfloat16)
    buffer = buffer.at[ids_blk, dest_rows].set(gated.reshape(GROUP, TOKENS_DEV, 2, D))
    return (hidden_out, buffer)
```

```python
import math
import jax
import jax.numpy as jnp
from jax import lax
from jax.experimental import pallas as pl
from jax.experimental.pallas import tpu as pltpu
from jax.sharding import PartitionSpec as P

MESH = pl.DeviceIdType.MESH
HEAD = 128
EXP_SCALE = math.log2(math.e) / math.sqrt(HEAD)
KC = 512
NC = 512
RING = 6
WO_BUFS = 4
AHEAD = 3
F32 = jnp.float32
BF16 = jnp.bfloat16


def block_kernel(x_ref, wq_ref, wk_ref, wv_ref, wo_ref, ids_ref, probs_ref,
                 h_ref, tab_ref,
                 xb, ring, wob, acc, kvacc, kv, ob, hb, oacc, mask, idsb, probsb, gsc, hsc, tabs,
                 ring_sem, wo_sem, loc_sem, xp_sem, xc_send, xc_recv, xr_send, xr_recv,
                 kv_sem, o_send, o_recv, hp_send, hp_recv, hc_send, hc_recv, hr_send, hr_recv,
                 t_send, t_recv, out_sem, tab_sem):
    tok, d = x_ref.shape
    own = 2 * tok
    rows = xb.shape[0]
    red = rows - own
    half = wq_ref.shape[1] // 2
    kvw = wk_ref.shape[1] // 2
    nk = d // KC
    per = half // (2 * kvw)
    n_kv = nk // per
    n_loads = n_kv + nk
    oh = d // 2
    nn = oh // NC
    groups = kvw // HEAD
    q_per = half // kvw
    gw = q_per * HEAD

    sp = lax.axis_index('sp')
    chip = sp // 2
    core = sp % 2
    partner = chip * 2 + (1 - core)
    across = (1 - chip) * 2 + core
    diag = (1 - chip) * 2 + (1 - core)

    def remote(src, dst, send, recv, dev):
        return pltpu.make_async_remote_copy(
            src_ref=src, dst_ref=dst, send_sem=send, recv_sem=recv,
            device_id={'sp': dev}, device_id_type=MESH)

    def load_kv(n):
        for j in range(per):
            r = pl.ds((n * per + j) * KC, KC)
            c = pl.ds(pl.multiple_of(core * kvw, HEAD), kvw)
            pltpu.make_async_copy(wk_ref.at[r, c], ring.at[n, :, pl.ds(2 * j * kvw, kvw)], ring_sem.at[n]).start()
            pltpu.make_async_copy(wv_ref.at[r, c], ring.at[n, :, pl.ds((2 * j + 1) * kvw, kvw)], ring_sem.at[n]).start()

    def load_q(n):
        slot = n % RING
        r = pl.ds(pl.multiple_of((n - n_kv) * KC, KC), KC)
        c = pl.ds(pl.multiple_of(core * half, HEAD), half)
        pltpu.make_async_copy(wq_ref.at[r, c], ring.at[slot], ring_sem.at[slot]).start()

    def wait_ring(slot):
        pltpu.make_async_copy(wq_ref.at[pl.ds(0, KC), pl.ds(0, half)], ring.at[slot], ring_sem.at[slot]).wait()

    def load_wo(n):
        slot = n % WO_BUFS
        c = pl.ds(pl.multiple_of(core * oh + n * NC, HEAD), NC)
        for side in range(2):
            r = pl.ds(pl.multiple_of((core if side == 0 else 1 - core) * half, HEAD), half)
            pltpu.make_async_copy(wo_ref.at[r, c], wob.at[slot, pl.ds(side * half, half), :], wo_sem.at[slot]).start()

    def wait_wo(slot):
        pltpu.make_async_copy(wo_ref.at[:, pl.ds(0, NC)], wob.at[slot], wo_sem.at[slot]).wait()

    own_rows = pl.ds(pl.multiple_of(core * tok, 16), tok)
    x_load = pltpu.make_async_copy(x_ref, xb.at[own_rows, :], loc_sem.at[0])
    ids_load = pltpu.make_async_copy(ids_ref, idsb, loc_sem.at[1])
    probs_load = pltpu.make_async_copy(probs_ref, probsb, loc_sem.at[2])
    x_load.start()
    ids_load.start()
    probs_load.start()
    for n in range(RING):
        if n < n_kv:
            load_kv(n)
        else:
            load_q(n)

    barrier = pltpu.get_barrier_semaphore()
    for dev in (partner, across, diag):
        pl.semaphore_signal(barrier, inc=1, device_id={'sp': dev}, device_id_type=MESH)
    pl.semaphore_wait(barrier, 3)

    x_load.wait()
    x_pair = remote(xb.at[own_rows, :], xb.at[own_rows, :], xp_sem.at[0], xp_sem.at[1], partner)
    x_pair.start()

    def x_cross(k):
        c = pl.ds(pl.multiple_of(k * KC, KC), KC)
        return remote(xb.at[pl.ds(0, red), c], xb.at[pl.ds(own, red), c], xc_send.at[k], xc_recv.at[k], across)

    def x_relay(k):
        c = pl.ds(pl.multiple_of(k * KC, KC), KC)
        part = xb.at[pl.ds(own, red), c]
        return remote(part, part, xr_send.at[k], xr_recv.at[k], partner)

    @pl.when(core == 0)
    def _():
        @pl.loop(0, nk)
        def _(k):
            x_cross(k).start()

    ids_load.wait()
    probs_load.wait()
    experts = probsb.shape[1]
    lane8 = lax.broadcasted_iota(jnp.int32, (tok, experts), 1)
    pr = probsb[...]
    hit0 = lane8 == idsb[:, 0:1]
    hit1 = lane8 == idsb[:, 1:2]
    p0 = jnp.sum(jnp.where(hit0, pr, 0.0), axis=1, keepdims=True)
    p1 = jnp.sum(jnp.where(hit1, pr, 0.0), axis=1, keepdims=True)
    hit = jnp.logical_or(hit0, hit1)
    gsc[...] = jnp.zeros_like(gsc)
    hsc[...] = jnp.zeros_like(hsc)
    gsc[0:tok, 0:experts] = jnp.where(hit, pr / (p0 + p1), 0.0)
    hsc[0:tok, 0:experts] = jnp.where(hit, 1.0, 0.0)
    mine = tabs.at[sp]
    tabs[sp, 0:experts, :] = jnp.transpose(gsc[...])[0:experts, :]
    tabs[sp, experts:2 * experts, :] = jnp.transpose(hsc[...])[0:experts, :]

    acc[...] = jnp.zeros_like(acc)
    kvacc[...] = jnp.zeros_like(kvacc)
    row = lax.broadcasted_iota(jnp.int32, (rows, 2 * own), 0)
    col = lax.broadcasted_iota(jnp.int32, (rows, 2 * own), 1)
    row_pos = jnp.where(row < own, row + chip * own, row - own + (1 - chip) * own)
    col_pos = jnp.where(col < own, col + chip * own, col - own + (1 - chip) * own)
    mask[...] = jnp.where(row_pos >= col_pos, 1.0, 0.0)

    tab_copies = [remote(mine, mine, t_send.at[i], t_recv.at[i], dev)
                  for i, dev in enumerate((partner, across, diag))]
    for copy in tab_copies:
        copy.start()

    x_pair.wait()

    @pl.loop(0, n_kv)
    def _(n):
        wait_ring(n)
        for j in range(per):
            c = pl.ds(pl.multiple_of((n * per + j) * KC, KC), KC)
            kvacc[...] += jnp.dot(xb[0:own, c], ring[n, :, 2 * j * kvw:2 * (j + 1) * kvw],
                                  preferred_element_type=F32)
        load_q(n + RING)

    kv[0:own, :] = kvacc[...].astype(BF16)

    for copy in tab_copies:
        copy.wait()
    tab_out = pltpu.make_async_copy(tabs, tab_ref, tab_sem)
    tab_out.start()

    kv_cross = remote(kv.at[pl.ds(0, own), :], kv.at[pl.ds(own, own), :], kv_sem.at[0], kv_sem.at[1], across)
    kv_cross.start()

    @pl.when(core == 0)
    def _():
        for k in range(AHEAD):
            x_cross(k).wait_recv()
            x_relay(k).start()

    @pl.loop(0, nk)
    def _(k):
        @pl.when(jnp.logical_and(core == 0, k + AHEAD < nk))
        def _():
            x_cross(k + AHEAD).wait_recv()
            x_relay(k + AHEAD).start()

        @pl.when(core == 1)
        def _():
            x_relay(k).wait_recv()

        n = n_kv + k
        slot = n % RING
        wait_ring(slot)
        c = pl.ds(pl.multiple_of(k * KC, KC), KC)
        acc[...] += jnp.dot(xb[:, c], ring[slot], preferred_element_type=F32)

        @pl.when(n + RING < n_loads)
        def _():
            load_q(n + RING)

        late = n + RING - n_loads
        for i, at in enumerate((0, 2, 4, 5)):
            @pl.when(late == at)
            def _():
                load_wo(i)

    kv_cross.wait()

    def o_pair(g):
        return remote(ob.at[:, pl.ds(pl.multiple_of(g * gw, HEAD), gw)],
                      ob.at[:, pl.ds(pl.multiple_of(half + g * gw, HEAD), gw)],
                      o_send.at[g], o_recv.at[g], partner)

    @pl.loop(0, groups)
    def _(g):
        kg = kv[:, pl.ds(pl.multiple_of(g * HEAD, HEAD), HEAD)]
        vg = kv[:, pl.ds(pl.multiple_of(kvw + g * HEAD, HEAD), HEAD)]
        for m in range(q_per):
            c = pl.ds(pl.multiple_of(g * gw + m * HEAD, HEAD), HEAD)
            s = lax.dot_general(acc[:, c].astype(BF16), kg, (((1,), (1,)), ((), ())),
                                preferred_element_type=F32)
            s = jnp.where(mask[...] > 0.5, s, -1e30)
            top = jnp.max(s, axis=1, keepdims=True)
            e = jnp.exp2((s - top) * EXP_SCALE)
            w = (e * (1.0 / jnp.sum(e, axis=1, keepdims=True))).astype(BF16)
            ob[:, c] = jnp.dot(w, vg, preferred_element_type=F32).astype(BF16)
        o_pair(g).start()

    def h_cols(side, n):
        return pl.ds(pl.multiple_of((core if side == 0 else 1 - core) * oh + n * NC, HEAD), NC)

    def h_pair(n):
        part = hb.at[pl.ds(0, rows), h_cols(0, n)]
        return remote(part, part, hp_send.at[n], hp_recv.at[n], partner)

    def h_cross(n):
        return remote(hb.at[pl.ds(red, own - red), h_cols(0, n)], hb.at[pl.ds(rows, own - red), h_cols(0, n)],
                      hc_send.at[n], hc_recv.at[n], across)

    def h_relay(n):
        part = hb.at[pl.ds(rows, own - red), h_cols(0, n)]
        return remote(part, part, hr_send.at[n], hr_recv.at[n], partner)

    def h_out(side, n):
        c = h_cols(side, n)
        return [pltpu.make_async_copy(
            hb.at[pl.ds(i * own, own), c],
            h_ref.at[pl.ds(pl.multiple_of((chip if i == 0 else 1 - chip) * own, 16), own), c],
            out_sem.at[side, n, i]) for i in range(2)]

    def relay_and_out(n):
        h_cross(n).wait_recv()
        h_relay(n).start()
        for copy in h_out(0, n):
            copy.start()

    def partner_out(n):
        h_pair(n).wait_recv()
        h_relay(n).wait_recv()
        for copy in h_out(1, n):
            copy.start()

    @pl.loop(0, nn)
    def _(n):
        slot = n % WO_BUFS
        wait_wo(slot)
        oacc[...] = jnp.dot(ob[:, 0:half], wob[slot, 0:half, :], preferred_element_type=F32)

        @pl.when(n == 0)
        def _():
            @pl.loop(0, groups)
            def _(g):
                o_pair(g).wait()

        part = oacc[...] + jnp.dot(ob[:, half:2 * half], wob[slot, half:2 * half, :], preferred_element_type=F32)
        hb[0:rows, h_cols(0, n)] = (xb[:, h_cols(0, n)].astype(F32) + part).astype(BF16)

        @pl.when(n + WO_BUFS < nn)
        def _():
            load_wo(n + WO_BUFS)

        h_cross(n).start()
        h_pair(n).start()

        @pl.when(n >= 2)
        def _():
            relay_and_out(n - 2)

        @pl.when(n >= 3)
        def _():
            partner_out(n - 3)

    relay_and_out(nn - 2)
    partner_out(nn - 3)
    relay_and_out(nn - 1)
    partner_out(nn - 2)
    partner_out(nn - 1)

    @pl.when(core == 0)
    def _():
        @pl.loop(0, nk)
        def _(k):
            x_cross(k).wait_send()
            x_relay(k).wait_send()

    @pl.loop(0, nn)
    def _(n):
        h_cross(n).wait_send()
        h_pair(n).wait_send()
        h_relay(n).wait_send()
        for side in range(2):
            for copy in h_out(side, n):
                copy.wait()

    tab_out.wait()


def dispatch_kernel(tab_ref, h_ref, hid_ref, buf_ref, pick, gate):
    sources, lines, lanes = tab_ref.shape
    experts = lines // 2
    tokens = h_ref.shape[0]
    tok = tokens // sources
    held = buf_ref.shape[0]
    sp = lax.axis_index('sp')

    @pl.when(pl.program_id(0) == 0)
    def _():
        before = lax.broadcasted_iota(jnp.int32, (lanes, lanes), 0) < lax.broadcasted_iota(jnp.int32, (lanes, lanes), 1)
        before = jnp.where(before, 1.0, 0.0).astype(BF16)
        dests, gates = [], []
        for s in range(sources):
            hits = tab_ref[s, experts:2 * experts, :]
            rank = jnp.dot(hits.astype(BF16), before, preferred_element_type=F32)
            dests.append(jnp.where(hits > 0.5, rank + (s * tok + 1.0), 0.0))
            gates.append(tab_ref[s, 0:experts, :])
        pair = lanes // tok
        line = lax.broadcasted_iota(jnp.int32, (experts, lanes), 0)
        slot = lax.broadcasted_iota(jnp.int32, (tokens, lanes), 0).astype(F32) + 1.0
        for e in range(held):
            total = jnp.zeros((tokens, 1), F32)
            for j in range(sources // pair):
                dest, g = dests[pair * j], gates[pair * j]
                for i in range(1, pair):
                    dest = dest + pltpu.roll(dests[pair * j + i], i * tok, 1)
                    g = g + pltpu.roll(gates[pair * j + i], i * tok, 1)
                mine = line == sp * held + e
                dest = jnp.sum(jnp.where(mine, dest, 0.0), axis=0, keepdims=True)
                g = jnp.sum(jnp.where(mine, g, 0.0), axis=0, keepdims=True)
                chosen = slot == dest
                pick[e * tokens:(e + 1) * tokens, j * lanes:(j + 1) * lanes] = jnp.where(chosen, 1.0, 0.0).astype(BF16)
                total = total + jnp.sum(jnp.where(chosen, g, 0.0), axis=1, keepdims=True)
            gate[e * tokens:(e + 1) * tokens, :] = total

    hid_ref[...] = h_ref[pl.ds(pl.multiple_of(sp * tok, 16), tok), :]
    for e in range(held):
        r = slice(e * tokens, (e + 1) * tokens)
        y = jnp.dot(pick[r, :], h_ref[...], preferred_element_type=F32)
        buf_ref[e] = (gate[r, :] * y).astype(BF16)


def solution(mesh):
    row_spec = P(('dp', 'sp'), None)
    buf_spec = P(('dp', 'sp'), None, None)
    group = mesh.shape['sp']

    def device_step(x, w_q, w_k, w_v, w_o, ids, probs):
        tok, d = x.shape
        half, kvw, oh = w_q.shape[1] // 2, w_k.shape[1] // 2, d // 2
        experts = probs.shape[1]
        own, tokens = 2 * tok, group * tok
        rows = own + tok
        nk, nn = d // KC, oh // NC
        any_spec = pl.BlockSpec(memory_space=pl.ANY)
        dma = pltpu.SemaphoreType.DMA
        h, tab = pl.pallas_call(
            block_kernel,
            out_shape=(jax.ShapeDtypeStruct((tokens, d), BF16),
                       jax.ShapeDtypeStruct((group, 2 * experts, 128), F32)),
            in_specs=[any_spec] * 7,
            out_specs=(any_spec, any_spec),
            scratch_shapes=[
                pltpu.VMEM((rows, d), BF16),
                pltpu.VMEM((RING, KC, half), BF16),
                pltpu.VMEM((WO_BUFS, d, NC), BF16),
                pltpu.VMEM((rows, half), F32),
                pltpu.VMEM((own, 2 * kvw), F32),
                pltpu.VMEM((tokens, 2 * kvw), BF16),
                pltpu.VMEM((rows, 2 * half), BF16),
                pltpu.VMEM((tokens, d), BF16),
                pltpu.VMEM((rows, NC), F32),
                pltpu.VMEM((rows, tokens), F32),
                pltpu.VMEM((tok, 2), jnp.int32),
                pltpu.VMEM((tok, experts), F32),
                pltpu.VMEM((128, 128), F32),
                pltpu.VMEM((128, 128), F32),
                pltpu.VMEM((group, 2 * experts, 128), F32),
                dma((RING,)), dma((WO_BUFS,)), dma((3,)), dma((2,)),
                dma((nk,)), dma((nk,)), dma((nk,)), dma((nk,)),
                dma((2,)), dma((kvw // HEAD,)), dma((kvw // HEAD,)),
                dma((nn,)), dma((nn,)), dma((nn,)), dma((nn,)), dma((nn,)), dma((nn,)),
                dma((3,)), dma((3,)), dma((2, nn, 2)), dma(()),
            ],
            compiler_params=pltpu.CompilerParams(
                collective_id=0, has_side_effects=True, vmem_limit_bytes=66_000_000),
            name='block',
        )(x, w_q, w_k, w_v, w_o, ids, probs)
        wide = 1024
        return pl.pallas_call(
            dispatch_kernel,
            grid=(d // wide,),
            out_shape=(jax.ShapeDtypeStruct((tok, d), BF16),
                       jax.ShapeDtypeStruct((experts // group, tokens, d), BF16)),
            in_specs=[pl.BlockSpec((group, 2 * experts, 128), lambda i: (0, 0, 0)),
                      pl.BlockSpec((tokens, wide), lambda i: (0, i))],
            out_specs=(pl.BlockSpec((tok, wide), lambda i: (0, i)),
                       pl.BlockSpec((experts // group, tokens, wide), lambda i: (0, 0, i))),
            scratch_shapes=[pltpu.VMEM((experts // group * tokens, tokens), BF16),
                            pltpu.VMEM((experts // group * tokens, 1), F32)],
            name='dispatch',
        )(tab, h)

    return jax.shard_map(device_step, mesh=mesh,
                         in_specs=(row_spec, P(), P(), P(), P(), row_spec, row_spec),
                         out_specs=(row_spec, buf_spec), check_vma=False)
```

```python
import math
import jax
import jax.numpy as jnp
from jax import lax
from jax.experimental import pallas as pl
from jax.experimental.pallas import tpu as pltpu
from jax.sharding import PartitionSpec as P

MESH = pl.DeviceIdType.MESH
HEAD = 128
SCALE = 1.0 / math.sqrt(HEAD)
EXP_SCALE = math.log2(math.e) * SCALE
MASKED = -1e30 / SCALE
KC = 1024
NC = 512
RING = 3
WO_BUFS = 4
AHEAD = 2
EARLY = 2
BLOCK_VMEM = 60_000_000
OUT_SPACE = pltpu.VMEM
F32 = jnp.float32
BF16 = jnp.bfloat16


def block_kernel(x_ref, wq_ref, wk_ref, wv_ref, wo_ref, ids_ref, probs_ref,
                 h_ref, pick_ref, gate_ref,
                 xb, ring, wob, acc, kvacc, kv, ob, oacc, mask, idsb, probsb, tabs,
                 ring_sem, wo_sem, loc_sem, xp_sem, xc_send, xc_recv, xr_send, xr_recv,
                 kv_sem, o_send, o_recv, hp_send, hp_recv, hc_send, hc_recv, hr_send, hr_recv,
                 t_send, t_recv):
    tok, d = x_ref.shape
    own = 2 * tok
    rows = xb.shape[0]
    red = rows - own
    half = wq_ref.shape[1] // 2
    kvw = wk_ref.shape[1] // 2
    nk = d // KC
    per = half // (2 * kvw)
    n_kv = nk // per
    n_loads = n_kv + nk
    oh = d // 2
    nn = oh // NC
    groups = kvw // HEAD
    q_per = half // kvw
    gw = q_per * HEAD

    sp = lax.axis_index('sp')
    chip = sp // 2
    core = sp % 2
    partner = chip * 2 + (1 - core)
    across = (1 - chip) * 2 + core
    diag = (1 - chip) * 2 + (1 - core)

    def remote(src, dst, send, recv, dev):
        return pltpu.make_async_remote_copy(
            src_ref=src, dst_ref=dst, send_sem=send, recv_sem=recv,
            device_id={'sp': dev}, device_id_type=MESH)

    def load_kv(n):
        for j in range(per):
            r = pl.ds((n * per + j) * KC, KC)
            c = pl.ds(pl.multiple_of(core * kvw, HEAD), kvw)
            pltpu.make_async_copy(wk_ref.at[r, c], ring.at[n, :, pl.ds(2 * j * kvw, kvw)], ring_sem.at[n]).start()
            pltpu.make_async_copy(wv_ref.at[r, c], ring.at[n, :, pl.ds((2 * j + 1) * kvw, kvw)], ring_sem.at[n]).start()

    def load_q(n):
        slot = n % RING
        r = pl.ds(pl.multiple_of((n - n_kv) * KC, KC), KC)
        c = pl.ds(pl.multiple_of(core * half, HEAD), half)
        pltpu.make_async_copy(wq_ref.at[r, c], ring.at[slot], ring_sem.at[slot]).start()

    def wait_ring(slot):
        pltpu.make_async_copy(wq_ref.at[pl.ds(0, KC), pl.ds(0, half)], ring.at[slot], ring_sem.at[slot]).wait()

    def load_wo(n):
        slot = n % WO_BUFS
        c = pl.ds(pl.multiple_of(core * oh + n * NC, HEAD), NC)
        for side in range(2):
            r = pl.ds(pl.multiple_of((core if side == 0 else 1 - core) * half, HEAD), half)
            pltpu.make_async_copy(wo_ref.at[r, c], wob.at[slot, pl.ds(side * half, half), :], wo_sem.at[slot]).start()

    def wait_wo(slot):
        pltpu.make_async_copy(wo_ref.at[:, pl.ds(0, NC)], wob.at[slot], wo_sem.at[slot]).wait()

    own_rows = pl.ds(pl.multiple_of(core * tok, 16), tok)
    x_load = pltpu.make_async_copy(x_ref, xb.at[own_rows, :], loc_sem.at[0])
    ids_load = pltpu.make_async_copy(ids_ref, idsb, loc_sem.at[1])
    probs_load = pltpu.make_async_copy(probs_ref, probsb, loc_sem.at[2])
    x_load.start()
    ids_load.start()
    probs_load.start()
    barrier = pltpu.get_barrier_semaphore()
    for dev in (partner, across, diag):
        pl.semaphore_signal(barrier, inc=1, device_id={'sp': dev}, device_id_type=MESH)
    with jax.named_scope('xl'):
        x_load.wait()
    for n in range(RING):
        if n < n_kv:
            load_kv(n)
        else:
            load_q(n)
    with jax.named_scope('bar'):
        pl.semaphore_wait(barrier, 3)

    x_pair = remote(xb.at[own_rows, :], xb.at[own_rows, :], xp_sem.at[0], xp_sem.at[1], partner)
    x_pair.start()

    def x_cross(k):
        c = pl.ds(pl.multiple_of(k * KC, KC), KC)
        return remote(xb.at[pl.ds(0, red), c], xb.at[pl.ds(own, red), c], xc_send.at[k], xc_recv.at[k], across)

    def x_relay(k):
        c = pl.ds(pl.multiple_of(k * KC, KC), KC)
        part = xb.at[pl.ds(own, red), c]
        return remote(part, part, xr_send.at[k], xr_recv.at[k], partner)

    @pl.when(core == 0)
    def _():
        for k in range(nk):
            x_cross(k).start()

    acc[...] = jnp.zeros_like(acc)
    kvacc[...] = jnp.zeros_like(kvacc)
    key = lax.broadcasted_iota(jnp.int32, (2 * own, 2 * own), 0)
    que = lax.broadcasted_iota(jnp.int32, (2 * own, 2 * own), 1)
    que = jnp.where(que < own, que, own + que % red)
    key_pos = jnp.where(key < own, key + chip * own, key - chip * own)
    que_pos = jnp.where(que < own, que + chip * own, que - chip * own)
    mask[...] = jnp.where(que_pos >= key_pos, 1.0, 0.0)
    ids_load.wait()
    probs_load.wait()
    experts = probsb.shape[0]
    line = lax.broadcasted_iota(jnp.int32, (experts, tok), 0)
    pr = probsb[...]
    hit0 = line == idsb[0:1, :]
    hit1 = line == idsb[1:2, :]
    p0 = jnp.sum(jnp.where(hit0, pr, 0.0), axis=0, keepdims=True)
    p1 = jnp.sum(jnp.where(hit1, pr, 0.0), axis=0, keepdims=True)
    hit = jnp.logical_or(hit0, hit1)
    tabs[sp] = jnp.zeros(tabs.shape[1:], F32)
    tabs[sp, 0:experts, 0:tok] = jnp.where(hit, pr / (p0 + p1), 0.0)
    tabs[sp, experts:2 * experts, 0:tok] = jnp.where(hit, 1.0, 0.0)

    with jax.named_scope('wxp'):
        x_pair.wait()

    @pl.loop(0, n_kv)
    def _(n):
        with jax.named_scope('wkv'):
            wait_ring(n)
        for j in range(per):
            c = pl.ds(pl.multiple_of((n * per + j) * KC, KC), KC)
            kvacc[...] += jnp.dot(xb[0:own, c], ring[n, :, 2 * j * kvw:2 * (j + 1) * kvw],
                                  preferred_element_type=F32)
        load_q(n + RING)

    kv[0:own, :] = kvacc[...].astype(BF16)
    kv_cross = remote(kv.at[pl.ds(0, own), :], kv.at[pl.ds(own, own), :], kv_sem.at[0], kv_sem.at[1], across)
    kv_cross.start()
    mine = tabs.at[sp]
    tab_copies = [remote(mine, mine, t_send.at[i], t_recv.at[i], dev)
                  for i, dev in enumerate((partner, across, diag))]
    for copy in tab_copies:
        copy.start()

    @pl.when(core == 0)
    def _():
        for k in range(AHEAD):
            with jax.named_scope('wxc0'):
                x_cross(k).wait_recv()
            x_relay(k).start()

    @pl.loop(0, nk)
    def _(k):
        @pl.when(jnp.logical_and(core == 0, k + AHEAD < nk))
        def _():
            with jax.named_scope('wxc'):
                x_cross(k + AHEAD).wait_recv()
            x_relay(k + AHEAD).start()

        @pl.when(core == 1)
        def _():
            with jax.named_scope('wxr'):
                x_relay(k).wait_recv()

        n = n_kv + k
        slot = n % RING
        with jax.named_scope('wq'):
            wait_ring(slot)
        c = pl.ds(pl.multiple_of(k * KC, KC), KC)
        acc[...] += jnp.dot(xb[:, c], ring[slot], preferred_element_type=F32)

        @pl.when(n + RING < n_loads)
        def _():
            load_q(n + RING)

        late = n + RING - n_loads
        for i, at in enumerate((0, 1, 2, 2)):
            @pl.when(late == at)
            def _():
                load_wo(i)

    with jax.named_scope('wkvx'):
        kv_cross.wait()

    def o_pair(g):
        return remote(ob.at[:, pl.ds(pl.multiple_of(g * gw, HEAD), gw)],
                      ob.at[:, pl.ds(pl.multiple_of(half + g * gw, HEAD), gw)],
                      o_send.at[g], o_recv.at[g], partner)

    @pl.loop(0, groups)
    def _(g):
        kg = kv[:, pl.ds(pl.multiple_of(g * HEAD, HEAD), HEAD)]
        vt = jnp.transpose(kv[:, pl.ds(pl.multiple_of(kvw + g * HEAD, HEAD), HEAD)])
        cols = [pl.ds(pl.multiple_of(g * gw + m * HEAD, HEAD), HEAD) for m in range(q_per)]
        q = jnp.concatenate([acc[0:own, c].astype(BF16) for c in cols]
                            + [acc[own:rows, c].astype(BF16) for c in cols], axis=0)
        seen = jnp.concatenate([mask[:, 0:own]] * q_per + [mask[:, own:2 * own]] * (q_per * red // own), axis=1)
        s = lax.dot_general(kg, q, (((1,), (1,)), ((), ())), preferred_element_type=F32)
        s = jnp.where(seen > 0.5, s, MASKED)
        top = jnp.max(s, axis=0, keepdims=True)
        e = jnp.exp2((s - top) * EXP_SCALE)
        w = (e * (1.0 / jnp.sum(e, axis=0, keepdims=True))).astype(BF16)
        o = jnp.transpose(jnp.dot(vt, w, preferred_element_type=F32)).astype(BF16)
        for m, c in enumerate(cols):
            ob[0:own, c] = o[m * own:(m + 1) * own, :]
            ob[own:rows, c] = o[q_per * own + m * red:q_per * own + (m + 1) * red, :]
        with jax.named_scope('os'):
            o_pair(g).start()

    def h_cols(side, n):
        return pl.ds(pl.multiple_of((core if side == 0 else 1 - core) * oh + n * NC, HEAD), NC)

    def h_pair(n):
        part = h_ref.at[pl.ds(0, rows), h_cols(0, n)]
        return remote(part, part, hp_send.at[n], hp_recv.at[n], partner)

    def h_cross(n):
        return remote(h_ref.at[pl.ds(red, own - red), h_cols(0, n)], h_ref.at[pl.ds(rows, own - red), h_cols(0, n)],
                      hc_send.at[n], hc_recv.at[n], across)

    def h_relay(n):
        part = h_ref.at[pl.ds(rows, own - red), h_cols(0, n)]
        return remote(part, part, hr_send.at[n], hr_recv.at[n], partner)

    def relay(n):
        with jax.named_scope('whc'):
            h_cross(n).wait_recv()
        h_relay(n).start()

    def finish(n, total):
        h_ref[0:rows, h_cols(0, n)] = (xb[:, h_cols(0, n)].astype(F32) + total).astype(BF16)

        @pl.when(n + WO_BUFS < nn)
        def _():
            load_wo(n + WO_BUFS)

        h_cross(n).start()
        h_pair(n).start()

    for n in range(EARLY):
        wait_wo(n)
        oacc[n] = jnp.dot(ob[:, 0:half], wob[n, 0:half, :], preferred_element_type=F32)

    with jax.named_scope('tab'):
        for copy in tab_copies:
            copy.wait()
    lanes = tabs.shape[2]
    held = pick_ref.shape[0] // pick_ref.shape[1]
    tokens = pick_ref.shape[1]
    before = lax.broadcasted_iota(jnp.int32, (lanes, lanes), 0) < lax.broadcasted_iota(jnp.int32, (lanes, lanes), 1)
    before = jnp.where(before, 1.0, 0.0).astype(BF16)
    dests, gates = [], []
    for j in range(2):
        dest, g = 0.0, 0.0
        for i in range(2):
            s = (chip if j == 0 else 1 - chip) * 2 + i
            hits = tabs[s, experts:2 * experts, :]
            rank = jnp.dot(hits.astype(BF16), before, preferred_element_type=F32)
            at = jnp.where(hits > 0.5, rank + (s * tok + 1).astype(F32), 0.0)
            gs = tabs[s, 0:experts, :]
            dest = dest + (at if i == 0 else pltpu.roll(at, tok, 1))
            g = g + (gs if i == 0 else pltpu.roll(gs, tok, 1))
        dests.append(dest)
        gates.append(g)
    line = lax.broadcasted_iota(jnp.int32, (experts, lanes), 0)
    slot = lax.broadcasted_iota(jnp.int32, (tokens, lanes), 0).astype(F32) + 1.0
    for e in range(held):
        total = jnp.zeros((tokens, 1), F32)
        for j in range(2):
            here = line == sp * held + e
            dest = jnp.sum(jnp.where(here, dests[j], 0.0), axis=0, keepdims=True)
            g = jnp.sum(jnp.where(here, gates[j], 0.0), axis=0, keepdims=True)
            chosen = slot == dest
            pick_ref[e * tokens:(e + 1) * tokens, j * lanes:(j + 1) * lanes] = jnp.where(chosen, 1.0, 0.0).astype(BF16)
            total = total + jnp.sum(jnp.where(chosen, g, 0.0), axis=1, keepdims=True)
        gate_ref[e * tokens:(e + 1) * tokens, :] = jnp.broadcast_to(total, (tokens, lanes))

    with jax.named_scope('wo'):
        @pl.loop(0, groups)
        def _(g):
            o_pair(g).wait()

    for n in range(EARLY):
        finish(n, oacc[n] + jnp.dot(ob[:, half:2 * half], wob[n, half:2 * half, :], preferred_element_type=F32))

    @pl.loop(EARLY, nn)
    def _(n):
        slot = n % WO_BUFS
        with jax.named_scope('wwo'):
            wait_wo(slot)
        finish(n, jnp.dot(ob[...], wob[slot], preferred_element_type=F32))
        relay(n - 2)

    relay(nn - 2)
    relay(nn - 1)

    @pl.when(core == 0)
    def _():
        @pl.loop(0, nk)
        def _(k):
            x_cross(k).wait_send()
            x_relay(k).wait_send()

    with jax.named_scope('end'):
        @pl.loop(0, nn)
        def _(n):
            h_cross(n).wait_send()
            h_pair(n).wait()
            h_relay(n).wait()


def dispatch_kernel(pick_ref, gate_ref, h_ref, hid_ref, buf_ref):
    tok, wide = hid_ref.shape
    held, tokens = buf_ref.shape[0], buf_ref.shape[1]
    core = lax.axis_index('sp') % 2
    c = pl.ds(pl.multiple_of(pl.program_id(0) * wide, wide), wide)
    hid_ref[...] = h_ref[pl.ds(pl.multiple_of(core * tok, 16), tok), c]
    for e in range(held):
        r = slice(e * tokens, (e + 1) * tokens)
        y = jnp.dot(pick_ref[r, :], h_ref[:, c], preferred_element_type=F32)
        g = gate_ref[r, :]
        for j in range(0, wide, HEAD):
            buf_ref[e, :, j:j + HEAD] = (g * y[:, j:j + HEAD]).astype(BF16)


def solution(mesh):
    row_spec = P(('dp', 'sp'), None)
    buf_spec = P(('dp', 'sp'), None, None)
    group = mesh.shape['sp']

    def device_step(x, w_q, w_k, w_v, w_o, ids, probs):
        tok, d = x.shape
        half, kvw, oh = w_q.shape[1] // 2, w_k.shape[1] // 2, d // 2
        experts = probs.shape[1]
        held = experts // group
        own, tokens = 2 * tok, group * tok
        rows = own + tok
        nk, nn = d // KC, oh // NC
        any_spec = pl.BlockSpec(memory_space=pl.ANY)
        vmem_spec = pl.BlockSpec(memory_space=pltpu.VMEM)
        dma = pltpu.SemaphoreType.DMA
        h, pick, gate = pl.pallas_call(
            block_kernel,
            out_shape=(OUT_SPACE((tokens, d), BF16),
                       OUT_SPACE((held * tokens, tokens), BF16),
                       OUT_SPACE((held * tokens, 128), F32)),
            in_specs=[any_spec] * 7,
            out_specs=(vmem_spec,) * 3,
            scratch_shapes=[
                pltpu.VMEM((rows, d), BF16),
                pltpu.VMEM((RING, KC, half), BF16),
                pltpu.VMEM((WO_BUFS, d, NC), BF16),
                pltpu.VMEM((rows, half), F32),
                pltpu.VMEM((own, 2 * kvw), F32),
                pltpu.VMEM((tokens, 2 * kvw), BF16),
                pltpu.VMEM((rows, 2 * half), BF16),
                pltpu.VMEM((EARLY, rows, NC), F32),
                pltpu.VMEM((tokens, tokens), F32),
                pltpu.VMEM((2, tok), jnp.int32),
                pltpu.VMEM((experts, tok), F32),
                pltpu.VMEM((group, 2 * experts, 128), F32),
                dma((RING,)), dma((WO_BUFS,)), dma((3,)), dma((2,)),
                dma((nk,)), dma((nk,)), dma((nk,)), dma((nk,)),
                dma((2,)), dma((kvw // HEAD,)), dma((kvw // HEAD,)),
                dma((nn,)), dma((nn,)), dma((nn,)), dma((nn,)), dma((nn,)), dma((nn,)),
                dma((3,)), dma((3,)),
            ],
            compiler_params=pltpu.CompilerParams(
                collective_id=0, has_side_effects=True, vmem_limit_bytes=BLOCK_VMEM),
            name='block',
        )(x, w_q, w_k, w_v, w_o, ids.T, probs.T)
        wide = 1024
        return pl.pallas_call(
            dispatch_kernel,
            grid=(d // wide,),
            out_shape=(jax.ShapeDtypeStruct((tok, d), BF16),
                       jax.ShapeDtypeStruct((held, tokens, d), BF16)),
            in_specs=[vmem_spec] * 3,
            out_specs=(pl.BlockSpec((tok, wide), lambda i: (0, i)),
                       pl.BlockSpec((held, tokens, wide), lambda i: (0, 0, i))),
            compiler_params=pltpu.CompilerParams(vmem_limit_bytes=16_000_000),
            name='dispatch',
        )(pick, gate, h)

    return jax.shard_map(device_step, mesh=mesh,
                         in_specs=(row_spec, P(), P(), P(), P(), row_spec, row_spec),
                         out_specs=(row_spec, buf_spec), check_vma=False)
```

```python
import math
import jax
import jax.numpy as jnp
from jax import lax
from jax.experimental import pallas as pl
from jax.experimental.pallas import tpu as pltpu
from jax.sharding import PartitionSpec as P

MESH = pl.DeviceIdType.MESH
HEAD = 128
SCALE = 1.0 / math.sqrt(HEAD)
EXP_SCALE = math.log2(math.e) * SCALE
MASKED = -1e30 / SCALE
KC = 1024
NC = 512
RING = 3
WO_BUFS = 4
AHEAD = 2
EARLY = 2
LAG = 3
KV_STEP = 3
PICK_STEP = 1
WIDE = 512
BLOCK_VMEM = 59_000_000
OUT_SPACE = pltpu.VMEM
F32 = jnp.float32
BF16 = jnp.bfloat16


def block_kernel(x_ref, wq_ref, wk_ref, wv_ref, wo_ref, ids_ref, probs_ref,
                 h_ref, pick_ref, gate_ref,
                 xb, ring, wob, acc, kvacc, kv, ob, oacc, idsb, probsb, tabs,
                 ring_sem, wo_sem, loc_sem, xp_sem, xc_send, xc_recv, xr_send, xr_recv,
                 kv_sem, o_send, o_recv, hp_send, hp_recv, hc_send, hc_recv, hr_send, hr_recv,
                 t_send, t_recv):
    tok, d = x_ref.shape
    own = 2 * tok
    rows = xb.shape[0]
    red = rows - own
    half = wq_ref.shape[1] // 2
    kvw = wk_ref.shape[1] // 2
    nk = d // KC
    per = half // (2 * kvw)
    n_kv = nk // per
    n_loads = n_kv + nk
    oh = d // 2
    nn = oh // NC
    groups = kvw // HEAD
    q_per = half // kvw
    gw = q_per * HEAD

    sp = lax.axis_index('sp')
    chip = sp // 2
    core = sp % 2
    partner = chip * 2 + (1 - core)
    across = (1 - chip) * 2 + core
    diag = (1 - chip) * 2 + (1 - core)

    def remote(src, dst, send, recv, dev):
        return pltpu.make_async_remote_copy(
            src_ref=src, dst_ref=dst, send_sem=send, recv_sem=recv,
            device_id={'sp': dev}, device_id_type=MESH)

    def load_kv(n):
        for j in range(per):
            r = pl.ds((n * per + j) * KC, KC)
            c = pl.ds(pl.multiple_of(core * kvw, HEAD), kvw)
            pltpu.make_async_copy(wk_ref.at[r, c], ring.at[n, :, pl.ds(2 * j * kvw, kvw)], ring_sem.at[n]).start()
            pltpu.make_async_copy(wv_ref.at[r, c], ring.at[n, :, pl.ds((2 * j + 1) * kvw, kvw)], ring_sem.at[n]).start()

    def load_q(n):
        slot = n % RING
        r = pl.ds(pl.multiple_of((n - n_kv) * KC, KC), KC)
        c = pl.ds(pl.multiple_of(core * half, HEAD), half)
        pltpu.make_async_copy(wq_ref.at[r, c], ring.at[slot], ring_sem.at[slot]).start()

    def wait_ring(slot):
        pltpu.make_async_copy(wq_ref.at[pl.ds(0, KC), pl.ds(0, half)], ring.at[slot], ring_sem.at[slot]).wait()

    def load_wo(n):
        slot = n % WO_BUFS
        c = pl.ds(pl.multiple_of(core * oh + n * NC, HEAD), NC)
        for side in range(2):
            r = pl.ds(pl.multiple_of((core if side == 0 else 1 - core) * half, HEAD), half)
            pltpu.make_async_copy(wo_ref.at[r, c], wob.at[slot, pl.ds(side * half, half), :], wo_sem.at[slot]).start()

    def wait_wo(slot):
        pltpu.make_async_copy(wo_ref.at[:, pl.ds(0, NC)], wob.at[slot], wo_sem.at[slot]).wait()

    own_rows = pl.ds(pl.multiple_of(core * tok, 16), tok)
    x_load = pltpu.make_async_copy(x_ref, xb.at[own_rows, :], loc_sem.at[0])
    for k in range(nk):
        c = pl.ds(k * KC, KC)
        pltpu.make_async_copy(x_ref.at[:, c], xb.at[own_rows, c], loc_sem.at[0]).start()
    ids_load = pltpu.make_async_copy(ids_ref, idsb, loc_sem.at[1])
    probs_load = pltpu.make_async_copy(probs_ref, probsb, loc_sem.at[2])
    ids_load.start()
    probs_load.start()
    load_kv(0)
    barrier = pltpu.get_barrier_semaphore()
    for dev in (partner, across, diag):
        pl.semaphore_signal(barrier, inc=1, device_id={'sp': dev}, device_id_type=MESH)
    with jax.named_scope('xl'):
        x_load.wait()
    for n in range(1, RING):
        if n < n_kv:
            load_kv(n)
        else:
            load_q(n)
    with jax.named_scope('bar'):
        pl.semaphore_wait(barrier, 3)

    x_pair = remote(xb.at[own_rows, :], xb.at[own_rows, :], xp_sem.at[0], xp_sem.at[1], partner)
    x_pair.start()

    def x_cross(k):
        c = pl.ds(pl.multiple_of(k * KC, KC), KC)
        return remote(xb.at[pl.ds(0, red), c], xb.at[pl.ds(own, red), c], xc_send.at[k], xc_recv.at[k], across)

    def x_relay(k):
        c = pl.ds(pl.multiple_of(k * KC, KC), KC)
        part = xb.at[pl.ds(own, red), c]
        return remote(part, part, xr_send.at[k], xr_recv.at[k], partner)

    ids_load.wait()
    probs_load.wait()
    experts = probsb.shape[0]
    line = lax.broadcasted_iota(jnp.int32, (experts, tok), 0)
    pr = probsb[...]
    hit0 = line == idsb[0:1, :]
    hit1 = line == idsb[1:2, :]
    p0 = jnp.sum(jnp.where(hit0, pr, 0.0), axis=0, keepdims=True)
    p1 = jnp.sum(jnp.where(hit1, pr, 0.0), axis=0, keepdims=True)
    hit = jnp.logical_or(hit0, hit1)
    tabs[sp] = jnp.zeros(tabs.shape[1:], F32)
    tabs[sp, 0:experts, 0:tok] = jnp.where(hit, pr / (p0 + p1), 0.0)
    tabs[sp, experts:2 * experts, 0:tok] = jnp.where(hit, 1.0, 0.0)
    mine = tabs.at[sp]
    tab_copies = [remote(mine, mine, t_send.at[i], t_recv.at[i], dev)
                  for i, dev in enumerate((partner, across, diag))]
    for copy in tab_copies:
        copy.start()

    @pl.when(core == 0)
    def _():
        for k in range(nk):
            x_cross(k).start()

    acc[...] = jnp.zeros_like(acc)
    kvacc[...] = jnp.zeros_like(kvacc)

    with jax.named_scope('wxp'):
        x_pair.wait()

    @pl.loop(0, n_kv)
    def _(n):
        with jax.named_scope('wkv'):
            wait_ring(n)
        for j in range(per):
            c = pl.ds(pl.multiple_of((n * per + j) * KC, KC), KC)
            kvacc[...] += jnp.dot(xb[0:own, c], ring[n, :, 2 * j * kvw:2 * (j + 1) * kvw],
                                  preferred_element_type=F32)
        load_q(n + RING)

    kv[0:own, :] = kvacc[...].astype(BF16)

    def kv_cross(count):
        return remote(kv.at[pl.ds(0, count), :], kv.at[pl.ds(own, count), :], kv_sem.at[0], kv_sem.at[1], across)

    def kv_send():
        @pl.when(chip == 0)
        def _():
            kv_cross(own).start()

        @pl.when(chip == 1)
        def _():
            kv_cross(red).start()


    def build_picks():
        with jax.named_scope('tab'):
            for copy in tab_copies:
                copy.wait()
        lanes = tabs.shape[2]
        tokens = pick_ref.shape[1]
        held = pick_ref.shape[0] // tokens
        before = lax.broadcasted_iota(jnp.int32, (lanes, lanes), 0) < lax.broadcasted_iota(jnp.int32, (lanes, lanes), 1)
        before = jnp.where(before, 1.0, 0.0).astype(BF16)
        dests, gates = [], []
        for j in range(2):
            dest, g = 0.0, 0.0
            for i in range(2):
                s = (chip if j == 0 else 1 - chip) * 2 + i
                hits = tabs[s, experts:2 * experts, :]
                rank = jnp.dot(hits.astype(BF16), before, preferred_element_type=F32)
                at = jnp.where(hits > 0.5, rank + (s * tok + 1).astype(F32), 0.0)
                gs = tabs[s, 0:experts, :]
                dest = dest + (at if i == 0 else pltpu.roll(at, tok, 1))
                g = g + (gs if i == 0 else pltpu.roll(gs, tok, 1))
            dests.append(dest)
            gates.append(g)
        line = lax.broadcasted_iota(jnp.int32, (experts, lanes), 0)
        slot = lax.broadcasted_iota(jnp.int32, (tokens, lanes), 0).astype(F32) + 1.0
        for e in range(held):
            total = jnp.zeros((tokens, 1), F32)
            for j in range(2):
                here = line == sp * held + e
                dest = jnp.sum(jnp.where(here, dests[j], 0.0), axis=0, keepdims=True)
                g = jnp.sum(jnp.where(here, gates[j], 0.0), axis=0, keepdims=True)
                chosen = slot == dest
                pick_ref[e * tokens:(e + 1) * tokens, j * lanes:(j + 1) * lanes] = jnp.where(chosen, 1.0, 0.0).astype(BF16)
                total = total + jnp.sum(jnp.where(chosen, g, 0.0), axis=1, keepdims=True)
            gate_ref[e * tokens:(e + 1) * tokens, :] = jnp.broadcast_to(total, (tokens, lanes))


    @pl.when(core == 0)
    def _():
        kv_send()
        for k in range(AHEAD):
            with jax.named_scope('wxc0'):
                x_cross(k).wait_recv()
            x_relay(k).start()

    @pl.loop(0, nk)
    def _(k):
        @pl.when(jnp.logical_and(core == 0, k + AHEAD < nk))
        def _():
            with jax.named_scope('wxc'):
                x_cross(k + AHEAD).wait_recv()
            x_relay(k + AHEAD).start()

        @pl.when(core == 1)
        def _():
            with jax.named_scope('wxr'):
                x_relay(k).wait_recv()

        @pl.when(jnp.logical_and(core == 1, k == KV_STEP))
        def _():
            kv_send()

        @pl.when(k == PICK_STEP)
        def _():
            build_picks()

        n = n_kv + k
        slot = n % RING
        with jax.named_scope('wq'):
            wait_ring(slot)
        c = pl.ds(pl.multiple_of(k * KC, KC), KC)
        acc[...] += jnp.dot(xb[:, c], ring[slot], preferred_element_type=F32)

        @pl.when(n + RING < n_loads)
        def _():
            load_q(n + RING)

        late = n + RING - n_loads
        for i, at in enumerate((0, 1, 2, 2)):
            @pl.when(late == at)
            def _():
                load_wo(i)

    def o_pair(g):
        return remote(ob.at[:, pl.ds(pl.multiple_of(g * gw, HEAD), gw)],
                      ob.at[:, pl.ds(pl.multiple_of(half + g * gw, HEAD), gw)],
                      o_send.at[g], o_recv.at[g], partner)

    def attend(r0, r1, g, first, last, tri):
        n = r1 - r0
        cols = [slice(g * gw + m * HEAD, g * gw + (m + 1) * HEAD) for m in range(q_per)]
        q = jnp.concatenate([acc[r0:r1, c].astype(BF16) for c in cols], axis=0)
        s = lax.dot_general(q, kv[first:last, g * HEAD:(g + 1) * HEAD], (((1,), (1,)), ((), ())),
                            preferred_element_type=F32)
        lo, hi = tri - first, tri - first + n
        que = lax.broadcasted_iota(jnp.int32, (q_per * n, n), 0) % n
        key = lax.broadcasted_iota(jnp.int32, (q_per * n, n), 1)
        parts = [s[:, :lo]] * (lo > 0) + [jnp.where(key <= que, s[:, lo:hi], MASKED)] + [s[:, hi:]] * (hi < last - first)
        s = jnp.concatenate(parts, axis=1)
        top = jnp.max(s, axis=1, keepdims=True)
        e = jnp.exp2((s - top) * EXP_SCALE)
        w = (e * (1.0 / jnp.sum(e, axis=1, keepdims=True))).astype(BF16)
        o = jnp.dot(w, kv[first:last, kvw + g * HEAD:kvw + (g + 1) * HEAD], preferred_element_type=F32).astype(BF16)
        for m, c in enumerate(cols):
            ob[r0:r1, c] = o[m * n:(m + 1) * n, :]

    def heads(own_keys, red_keys):
        for g in range(groups):
            attend(0, own, g, *own_keys, 0)
            attend(own, rows, g, *red_keys, own)
            with jax.named_scope('os'):
                o_pair(g).start()

    @pl.when(chip == 0)
    def _():
        with jax.named_scope('wkvx'):
            kv_cross(red).wait_recv()
        heads((0, own), (0, own + red))

    @pl.when(chip == 1)
    def _():
        with jax.named_scope('wkvx'):
            kv_cross(own).wait_recv()
        heads((0, 2 * own), (own, own + red))

    def h_cols(side, n):
        return pl.ds(pl.multiple_of((core if side == 0 else 1 - core) * oh + n * NC, HEAD), NC)

    def h_pair(n):
        part = h_ref.at[pl.ds(0, rows), h_cols(0, n)]
        return remote(part, part, hp_send.at[n], hp_recv.at[n], partner)

    def h_cross(n):
        return remote(h_ref.at[pl.ds(red, own - red), h_cols(0, n)], h_ref.at[pl.ds(rows, own - red), h_cols(0, n)],
                      hc_send.at[n], hc_recv.at[n], across)

    def h_relay(n):
        part = h_ref.at[pl.ds(rows, own - red), h_cols(0, n)]
        return remote(part, part, hr_send.at[n], hr_recv.at[n], partner)

    def relay(n):
        with jax.named_scope('whc'):
            h_cross(n).wait_recv()
        h_relay(n).start()

    def finish(n, total):
        h_ref[0:rows, h_cols(0, n)] = (xb[:, h_cols(0, n)].astype(F32) + total).astype(BF16)

        @pl.when(n + WO_BUFS < nn)
        def _():
            load_wo(n + WO_BUFS)

        h_cross(n).start()
        h_pair(n).start()

    for n in range(EARLY):
        wait_wo(n)
        oacc[n] = jnp.dot(ob[:, 0:half], wob[n, 0:half, :], preferred_element_type=F32)

    with jax.named_scope('wo'):
        @pl.loop(0, groups)
        def _(g):
            o_pair(g).wait()

    for n in range(EARLY):
        finish(n, oacc[n] + jnp.dot(ob[:, half:2 * half], wob[n, half:2 * half, :], preferred_element_type=F32))

    @pl.loop(EARLY, nn)
    def _(n):
        slot = n % WO_BUFS
        with jax.named_scope('wwo'):
            wait_wo(slot)
        finish(n, jnp.dot(ob[...], wob[slot], preferred_element_type=F32))

        @pl.when(n >= LAG)
        def _():
            relay(n - LAG)

    for n in range(LAG):
        relay(nn - LAG + n)

    @pl.when(core == 0)
    def _():
        @pl.loop(0, nk)
        def _(k):
            x_cross(k).wait_send()
            x_relay(k).wait_send()

    @pl.when(chip == 0)
    def _():
        kv_cross(own).wait_send()

    @pl.when(chip == 1)
    def _():
        kv_cross(red).wait_send()

    with jax.named_scope('end'):
        @pl.loop(0, nn)
        def _(n):
            h_cross(n).wait_send()
            h_pair(n).wait()
            h_relay(n).wait()


def dispatch_kernel(pick_ref, gate_ref, h_ref, hid_ref, buf_ref, out, sems):
    tok, d = hid_ref.shape
    held, tokens = buf_ref.shape[0], buf_ref.shape[1]
    core = lax.axis_index('sp') % 2
    own_rows = pl.ds(pl.multiple_of(core * tok, 16), tok)
    copies = [pltpu.make_async_copy(h_ref.at[own_rows, :], hid_ref, sems.at[0])]
    copies[0].start()
    for i in range(d // WIDE):
        c = slice(i * WIDE, (i + 1) * WIDE)
        y = jnp.dot(pick_ref[...], h_ref[:, c], preferred_element_type=F32)
        for e in range(held):
            r = slice(e * tokens, (e + 1) * tokens)
            g = gate_ref[r, :]
            for j in range(0, WIDE, HEAD):
                out[e, :, i * WIDE + j:i * WIDE + j + HEAD] = (g * y[r, j:j + HEAD]).astype(BF16)
        part = pl.ds(i * WIDE, WIDE)
        copy = pltpu.make_async_copy(out.at[:, :, part], buf_ref.at[:, :, part], sems.at[1 + i])
        copy.start()
        copies.append(copy)
    for copy in copies:
        copy.wait()


def solution(mesh):
    row_spec = P(('dp', 'sp'), None)
    buf_spec = P(('dp', 'sp'), None, None)
    group = mesh.shape['sp']

    def device_step(x, w_q, w_k, w_v, w_o, ids, probs):
        tok, d = x.shape
        half, kvw, oh = w_q.shape[1] // 2, w_k.shape[1] // 2, d // 2
        experts = probs.shape[1]
        held = experts // group
        own, tokens = 2 * tok, group * tok
        rows = own + tok
        nk, nn = d // KC, oh // NC
        any_spec = pl.BlockSpec(memory_space=pl.ANY)
        vmem_spec = pl.BlockSpec(memory_space=pltpu.VMEM)
        dma = pltpu.SemaphoreType.DMA
        h, pick, gate = pl.pallas_call(
            block_kernel,
            out_shape=(OUT_SPACE((tokens, d), BF16),
                       OUT_SPACE((held * tokens, tokens), BF16),
                       OUT_SPACE((held * tokens, 128), F32)),
            in_specs=[any_spec] * 7,
            out_specs=(vmem_spec,) * 3,
            scratch_shapes=[
                pltpu.VMEM((rows, d), BF16),
                pltpu.VMEM((RING, KC, half), BF16),
                pltpu.VMEM((WO_BUFS, d, NC), BF16),
                pltpu.VMEM((rows, half), F32),
                pltpu.VMEM((own, 2 * kvw), F32),
                pltpu.VMEM((tokens, 2 * kvw), BF16),
                pltpu.VMEM((rows, 2 * half), BF16),
                pltpu.VMEM((EARLY, rows, NC), F32),
                pltpu.VMEM((2, tok), jnp.int32),
                pltpu.VMEM((experts, tok), F32),
                pltpu.VMEM((group, 2 * experts, 128), F32),
                dma((RING,)), dma((WO_BUFS,)), dma((3,)), dma((2,)),
                dma((nk,)), dma((nk,)), dma((nk,)), dma((nk,)),
                dma((2,)), dma((kvw // HEAD,)), dma((kvw // HEAD,)),
                dma((nn,)), dma((nn,)), dma((nn,)), dma((nn,)), dma((nn,)), dma((nn,)),
                dma((3,)), dma((3,)),
            ],
            compiler_params=pltpu.CompilerParams(
                collective_id=0, has_side_effects=True, vmem_limit_bytes=BLOCK_VMEM),
            name='block',
        )(x, w_q, w_k, w_v, w_o, ids.T, probs.T)
        return pl.pallas_call(
            dispatch_kernel,
            out_shape=(jax.ShapeDtypeStruct((tok, d), BF16),
                       jax.ShapeDtypeStruct((held, tokens, d), BF16)),
            in_specs=[vmem_spec] * 3,
            out_specs=(any_spec,) * 2,
            scratch_shapes=[pltpu.VMEM((held, tokens, d), BF16), dma((1 + d // WIDE,))],
            compiler_params=pltpu.CompilerParams(vmem_limit_bytes=16_000_000),
            name='dispatch',
        )(pick, gate, h)

    return jax.shard_map(device_step, mesh=mesh,
                         in_specs=(row_spec, P(), P(), P(), P(), row_spec, row_spec),
                         out_specs=(row_spec, buf_spec), check_vma=False)
```

```python
import math
import jax
import jax.numpy as jnp
from jax import lax
from jax.experimental import pallas as pl
from jax.experimental.pallas import tpu as pltpu
from jax.sharding import PartitionSpec as P

MESH = pl.DeviceIdType.MESH
HEAD = 128
SCALE = 1.0 / math.sqrt(HEAD)
EXP_SCALE = math.log2(math.e) * SCALE
MASKED = -1e30 / SCALE
KC = 1024
NC = 512
RING = 3
WO_BUFS = 4
AHEAD = 1
EARLY = 2
LAG = 3
KV_STEP = 3
PICK_STEP = 3
WIDE = 512
BLOCK_VMEM = 59_000_000
OUT_SPACE = pltpu.VMEM
F32 = jnp.float32
BF16 = jnp.bfloat16


def block_kernel(x_ref, wq_ref, wk_ref, wv_ref, wo_ref, ids_ref, probs_ref,
                 h_ref, pick_ref, gate_ref,
                 xb, ring, wob, acc, kvacc, kv, ob, oacc, idsb, probsb, tabs,
                 ring_sem, wo_sem, loc_sem, xp_sem, xc_send, xc_recv, xr_send, xr_recv,
                 kv_sem, o_sem, hp_sem, hc_send, hc_recv, hr_sem, t_sem):
    tok, d = x_ref.shape
    own = 2 * tok
    rows = xb.shape[0]
    red = rows - own
    half = wq_ref.shape[1] // 2
    kvw = wk_ref.shape[1] // 2
    nk = d // KC
    per = half // (2 * kvw)
    n_kv = nk // per
    n_loads = n_kv + nk
    oh = d // 2
    nn = oh // NC
    groups = kvw // HEAD
    q_per = half // kvw
    gw = q_per * HEAD

    sp = lax.axis_index('sp')
    chip = sp // 2
    core = sp % 2
    partner = chip * 2 + (1 - core)
    across = (1 - chip) * 2 + core
    diag = (1 - chip) * 2 + (1 - core)

    def remote(src, dst, send, recv, dev):
        return pltpu.make_async_remote_copy(
            src_ref=src, dst_ref=dst, send_sem=send, recv_sem=recv,
            device_id={'sp': dev}, device_id_type=MESH)

    def load_kv(n):
        for j in range(per):
            r = pl.ds((n * per + j) * KC, KC)
            c = pl.ds(pl.multiple_of(core * kvw, HEAD), kvw)
            pltpu.make_async_copy(wk_ref.at[r, c], ring.at[n, :, pl.ds(2 * j * kvw, kvw)], ring_sem.at[n]).start()
            pltpu.make_async_copy(wv_ref.at[r, c], ring.at[n, :, pl.ds((2 * j + 1) * kvw, kvw)], ring_sem.at[n]).start()

    def load_q(n):
        slot = n % RING
        r = pl.ds(pl.multiple_of((n - n_kv) * KC, KC), KC)
        c = pl.ds(pl.multiple_of(core * half, HEAD), half)
        pltpu.make_async_copy(wq_ref.at[r, c], ring.at[slot], ring_sem.at[slot]).start()

    def wait_ring(slot):
        pltpu.make_async_copy(wq_ref.at[pl.ds(0, KC), pl.ds(0, half)], ring.at[slot], ring_sem.at[slot]).wait()

    def load_wo(n):
        slot = n % WO_BUFS
        c = pl.ds(pl.multiple_of(core * oh + n * NC, HEAD), NC)
        for side in range(2):
            r = pl.ds(pl.multiple_of((core if side == 0 else 1 - core) * half, HEAD), half)
            pltpu.make_async_copy(wo_ref.at[r, c], wob.at[slot, pl.ds(side * half, half), :], wo_sem.at[slot]).start()

    def wait_wo(slot):
        pltpu.make_async_copy(wo_ref.at[:, pl.ds(0, NC)], wob.at[slot], wo_sem.at[slot]).wait()

    barrier = pltpu.get_barrier_semaphore()
    for dev in (partner, across, diag):
        pl.semaphore_signal(barrier, inc=1, device_id={'sp': dev}, device_id_type=MESH)

    own_rows = pl.ds(pl.multiple_of(core * tok, 16), tok)
    x_load = pltpu.make_async_copy(x_ref, xb.at[own_rows, :], loc_sem.at[0])
    ids_load = pltpu.make_async_copy(ids_ref, idsb, loc_sem.at[1])
    probs_load = pltpu.make_async_copy(probs_ref, probsb, loc_sem.at[2])
    x_load.start()
    ids_load.start()
    probs_load.start()
    load_kv(0)

    with jax.named_scope('bar'):
        pl.semaphore_wait(barrier, 3)

    x_pair = remote(x_ref, xb.at[own_rows, :], xp_sem.at[0], xp_sem.at[1], partner)
    x_pair.start()

    def x_cross(k):
        c = pl.ds(pl.multiple_of(k * KC, KC), KC)
        return remote(x_ref.at[:, c], xb.at[pl.ds(own, red), c], xc_send, xc_recv.at[k], across)

    def x_relay(k):
        c = pl.ds(pl.multiple_of(k * KC, KC), KC)
        part = xb.at[pl.ds(own, red), c]
        return remote(part, part, xr_send, xr_recv.at[k], partner)

    @pl.when(core == 0)
    def _():
        for k in range(nk):
            x_cross(k).start()

    with jax.named_scope('xl'):
        x_load.wait()
    for n in range(1, RING):
        if n < n_kv:
            load_kv(n)
        else:
            load_q(n)

    ids_load.wait()
    probs_load.wait()
    experts = probsb.shape[0]
    line = lax.broadcasted_iota(jnp.int32, (experts, tok), 0)
    pr = probsb[...]
    hit0 = line == idsb[0:1, :]
    hit1 = line == idsb[1:2, :]
    p0 = jnp.sum(jnp.where(hit0, pr, 0.0), axis=0, keepdims=True)
    p1 = jnp.sum(jnp.where(hit1, pr, 0.0), axis=0, keepdims=True)
    hit = jnp.logical_or(hit0, hit1)
    tabs[sp] = jnp.zeros(tabs.shape[1:], F32)
    tabs[sp, 0:experts, 0:tok] = jnp.where(hit, pr / (p0 + p1), 0.0)
    tabs[sp, experts:2 * experts, 0:tok] = jnp.where(hit, 1.0, 0.0)
    mine = tabs.at[sp]
    tab_copies = [remote(mine, mine, t_sem.at[0], t_sem.at[1], dev)
                  for i, dev in enumerate((partner, across, diag))]
    for copy in tab_copies:
        copy.start()

    acc[...] = jnp.zeros_like(acc)
    kvacc[...] = jnp.zeros_like(kvacc)

    with jax.named_scope('wxp'):
        x_pair.wait()

    @pl.loop(0, n_kv)
    def _(n):
        with jax.named_scope('wkv'):
            wait_ring(n)
        for j in range(per):
            c = pl.ds(pl.multiple_of((n * per + j) * KC, KC), KC)
            kvacc[...] += jnp.dot(xb[0:own, c], ring[n, :, 2 * j * kvw:2 * (j + 1) * kvw],
                                  preferred_element_type=F32)
        load_q(n + RING)

    kv[0:own, :] = kvacc[...].astype(BF16)

    def kv_cross(count):
        return remote(kv.at[pl.ds(0, count), :], kv.at[pl.ds(own, count), :], kv_sem.at[0], kv_sem.at[1], across)

    def kv_send():
        @pl.when(chip == 0)
        def _():
            kv_cross(own).start()

        @pl.when(chip == 1)
        def _():
            kv_cross(red).start()


    def build_picks():
        with jax.named_scope('tab'):
            three = tabs.at[pl.ds(0, 3)]
            remote(three, three, t_sem.at[0], t_sem.at[1], partner).wait()
        lanes = tabs.shape[2]
        tokens = pick_ref.shape[1]
        held = pick_ref.shape[0] // tokens
        before = lax.broadcasted_iota(jnp.int32, (lanes, lanes), 0) < lax.broadcasted_iota(jnp.int32, (lanes, lanes), 1)
        before = jnp.where(before, 1.0, 0.0).astype(BF16)
        dests, gates = [], []
        for j in range(2):
            dest, g = 0.0, 0.0
            for i in range(2):
                s = (chip if j == 0 else 1 - chip) * 2 + i
                hits = tabs[s, experts:2 * experts, :]
                rank = jnp.dot(hits.astype(BF16), before, preferred_element_type=F32)
                at = jnp.where(hits > 0.5, rank + (s * tok + 1).astype(F32), 0.0)
                gs = tabs[s, 0:experts, :]
                dest = dest + (at if i == 0 else pltpu.roll(at, tok, 1))
                g = g + (gs if i == 0 else pltpu.roll(gs, tok, 1))
            dests.append(dest)
            gates.append(g)
        line = lax.broadcasted_iota(jnp.int32, (experts, lanes), 0)
        slot = lax.broadcasted_iota(jnp.int32, (tokens, lanes), 0).astype(F32) + 1.0
        for e in range(held):
            total = jnp.zeros((tokens, 1), F32)
            for j in range(2):
                here = line == sp * held + e
                dest = jnp.sum(jnp.where(here, dests[j], 0.0), axis=0, keepdims=True)
                g = jnp.sum(jnp.where(here, gates[j], 0.0), axis=0, keepdims=True)
                chosen = slot == dest
                pick_ref[e * tokens:(e + 1) * tokens, j * lanes:(j + 1) * lanes] = jnp.where(chosen, 1.0, 0.0).astype(BF16)
                total = total + jnp.sum(jnp.where(chosen, g, 0.0), axis=1, keepdims=True)
            gate_ref[e * tokens:(e + 1) * tokens, :] = jnp.broadcast_to(total, (tokens, lanes))


    @pl.when(core == 0)
    def _():
        kv_send()
        for k in range(AHEAD):
            with jax.named_scope('wxc0'):
                x_cross(k).wait_recv()
            x_relay(k).start()

    @pl.loop(0, nk)
    def _(k):
        @pl.when(jnp.logical_and(core == 0, k + AHEAD < nk))
        def _():
            with jax.named_scope('wxc'):
                x_cross(k + AHEAD).wait_recv()
            x_relay(k + AHEAD).start()

        @pl.when(core == 1)
        def _():
            with jax.named_scope('wxr'):
                x_relay(k).wait_recv()

        @pl.when(jnp.logical_and(core == 1, k == KV_STEP))
        def _():
            kv_send()

        @pl.when(k == PICK_STEP)
        def _():
            build_picks()

        n = n_kv + k
        slot = n % RING
        with jax.named_scope('wq'):
            wait_ring(slot)
        c = pl.ds(pl.multiple_of(k * KC, KC), KC)
        acc[...] += jnp.dot(xb[:, c], ring[slot], preferred_element_type=F32)

        @pl.when(n + RING < n_loads)
        def _():
            load_q(n + RING)

        late = n + RING - n_loads
        for i, at in enumerate((1, 2, 2, 2)):
            @pl.when(late == at)
            def _():
                load_wo(i)

    def o_pair(first, count):
        return remote(ob.at[:, pl.ds(first * gw, count * gw)], ob.at[:, pl.ds(half + first * gw, count * gw)],
                      o_sem.at[0], o_sem.at[1], partner)

    def attend(r0, r1, g, first, last, tri):
        n = r1 - r0
        cols = [slice(g * gw + m * HEAD, g * gw + (m + 1) * HEAD) for m in range(q_per)]
        q = jnp.concatenate([acc[r0:r1, c].astype(BF16) for c in cols], axis=0)
        s = lax.dot_general(q, kv[first:last, g * HEAD:(g + 1) * HEAD], (((1,), (1,)), ((), ())),
                            preferred_element_type=F32)
        lo, hi = tri - first, tri - first + n
        que = lax.broadcasted_iota(jnp.int32, (q_per * n, n), 0) % n
        key = lax.broadcasted_iota(jnp.int32, (q_per * n, n), 1)
        parts = [s[:, :lo]] * (lo > 0) + [jnp.where(key <= que, s[:, lo:hi], MASKED)] + [s[:, hi:]] * (hi < last - first)
        s = jnp.concatenate(parts, axis=1)
        top = jnp.max(s, axis=1, keepdims=True)
        e = jnp.exp2((s - top) * EXP_SCALE)
        w = (e * (1.0 / jnp.sum(e, axis=1, keepdims=True))).astype(BF16)
        o = jnp.dot(w, kv[first:last, kvw + g * HEAD:kvw + (g + 1) * HEAD], preferred_element_type=F32).astype(BF16)
        for m, c in enumerate(cols):
            ob[r0:r1, c] = o[m * n:(m + 1) * n, :]

    def heads(own_keys, red_keys):
        for g in range(groups):
            attend(0, own, g, *own_keys, 0)
            attend(own, rows, g, *red_keys, own)
            if g == groups - 2:
                with jax.named_scope('os'):
                    o_pair(0, groups - 1).start()
        with jax.named_scope('os'):
            o_pair(groups - 1, 1).start()

    @pl.when(chip == 0)
    def _():
        with jax.named_scope('wkvx'):
            kv_cross(red).wait_recv()
        heads((0, own), (0, own + red))

    @pl.when(chip == 1)
    def _():
        with jax.named_scope('wkvx'):
            kv_cross(own).wait_recv()
        heads((0, 2 * own), (own, own + red))

    def h_cols(side, n):
        return pl.ds(pl.multiple_of((core if side == 0 else 1 - core) * oh + n * NC, HEAD), NC)

    def h_pair(n):
        part = h_ref.at[pl.ds(0, rows), h_cols(0, n)]
        return remote(part, part, hp_sem.at[0], hp_sem.at[1], partner)

    def h_cross(n):
        return remote(h_ref.at[pl.ds(red, own - red), h_cols(0, n)], h_ref.at[pl.ds(rows, own - red), h_cols(0, n)],
                      hc_send, hc_recv.at[n], across)

    def h_relay(n):
        part = h_ref.at[pl.ds(rows, own - red), h_cols(0, n)]
        return remote(part, part, hr_sem.at[0], hr_sem.at[1], partner)

    def relay(n):
        with jax.named_scope('whc'):
            h_cross(n).wait_recv()
        h_relay(n).start()

    def finish(n, total):
        h_ref[0:rows, h_cols(0, n)] = (xb[:, h_cols(0, n)].astype(F32) + total).astype(BF16)

        @pl.when(n + WO_BUFS < nn)
        def _():
            load_wo(n + WO_BUFS)

        h_cross(n).start()
        h_pair(n).start()

    for n in range(EARLY):
        wait_wo(n)
        oacc[n] = jnp.dot(ob[:, 0:half], wob[n, 0:half, :], preferred_element_type=F32)

    with jax.named_scope('wo'):
        o_pair(0, groups).wait()

    for n in range(EARLY):
        finish(n, oacc[n] + jnp.dot(ob[:, half:2 * half], wob[n, half:2 * half, :], preferred_element_type=F32))

    @pl.loop(EARLY, nn)
    def _(n):
        slot = n % WO_BUFS
        with jax.named_scope('wwo'):
            wait_wo(slot)
        finish(n, jnp.dot(ob[...], wob[slot], preferred_element_type=F32))

        @pl.when(n >= LAG)
        def _():
            relay(n - LAG)

    for n in range(LAG):
        relay(nn - LAG + n)

    @pl.when(core == 0)
    def _():
        part = xb.at[pl.ds(own, red), :]
        remote(x_ref, part, xc_send, xc_recv.at[0], across).wait_send()
        remote(part, part, xr_send, xr_recv.at[0], partner).wait_send()

    @pl.when(chip == 0)
    def _():
        kv_cross(own).wait_send()

    @pl.when(chip == 1)
    def _():
        kv_cross(red).wait_send()

    with jax.named_scope('end'):
        shared = h_ref.at[pl.ds(0, rows), pl.ds(0, oh)]
        late = h_ref.at[pl.ds(rows, own - red), pl.ds(0, oh)]
        remote(late, late, hc_send, hc_recv.at[0], across).wait_send()
        remote(shared, shared, hp_sem.at[0], hp_sem.at[1], partner).wait()
        remote(late, late, hr_sem.at[0], hr_sem.at[1], partner).wait()


def dispatch_kernel(pick_ref, gate_ref, h_ref, hid_ref, buf_ref, out, sems):
    tok, d = hid_ref.shape
    held, tokens = buf_ref.shape[0], buf_ref.shape[1]
    core = lax.axis_index('sp') % 2
    own_rows = pl.ds(pl.multiple_of(core * tok, 16), tok)
    copies = [pltpu.make_async_copy(h_ref.at[own_rows, :], hid_ref, sems.at[0])]
    copies[0].start()
    for i in range(d // WIDE):
        c = slice(i * WIDE, (i + 1) * WIDE)
        y = jnp.dot(pick_ref[...], h_ref[:, c], preferred_element_type=F32)
        for e in range(held):
            r = slice(e * tokens, (e + 1) * tokens)
            g = gate_ref[r, :]
            for j in range(0, WIDE, HEAD):
                out[e, :, i * WIDE + j:i * WIDE + j + HEAD] = (g * y[r, j:j + HEAD]).astype(BF16)
        part = pl.ds(i * WIDE, WIDE)
        copy = pltpu.make_async_copy(out.at[:, :, part], buf_ref.at[:, :, part], sems.at[1 + i])
        copy.start()
        copies.append(copy)
    for copy in copies:
        copy.wait()


def solution(mesh):
    row_spec = P(('dp', 'sp'), None)
    buf_spec = P(('dp', 'sp'), None, None)
    group = mesh.shape['sp']

    def device_step(x, w_q, w_k, w_v, w_o, ids, probs):
        tok, d = x.shape
        half, kvw, oh = w_q.shape[1] // 2, w_k.shape[1] // 2, d // 2
        experts = probs.shape[1]
        held = experts // group
        own, tokens = 2 * tok, group * tok
        rows = own + tok
        nk, nn = d // KC, oh // NC
        any_spec = pl.BlockSpec(memory_space=pl.ANY)
        vmem_spec = pl.BlockSpec(memory_space=pltpu.VMEM)
        dma = pltpu.SemaphoreType.DMA
        h, pick, gate = pl.pallas_call(
            block_kernel,
            out_shape=(OUT_SPACE((tokens, d), BF16),
                       OUT_SPACE((held * tokens, tokens), BF16),
                       OUT_SPACE((held * tokens, 128), F32)),
            in_specs=[any_spec] * 7,
            out_specs=(vmem_spec,) * 3,
            scratch_shapes=[
                pltpu.VMEM((rows, d), BF16),
                pltpu.VMEM((RING, KC, half), BF16),
                pltpu.VMEM((WO_BUFS, d, NC), BF16),
                pltpu.VMEM((rows, half), F32),
                pltpu.VMEM((own, 2 * kvw), F32),
                pltpu.VMEM((tokens, 2 * kvw), BF16),
                pltpu.VMEM((rows, 2 * half), BF16),
                pltpu.VMEM((EARLY, rows, NC), F32),
                pltpu.VMEM((2, tok), jnp.int32),
                pltpu.VMEM((experts, tok), F32),
                pltpu.VMEM((group, 2 * experts, 128), F32),
                dma((RING,)), dma((WO_BUFS,)), dma((3,)), dma((2,)),
                dma(()), dma((nk,)), dma(()), dma((nk,)),
                dma((2,)), dma((2,)), dma((2,)), dma(()), dma((nn,)), dma((2,)), dma((2,)),
            ],
            compiler_params=pltpu.CompilerParams(
                collective_id=0, has_side_effects=True, vmem_limit_bytes=BLOCK_VMEM),
            name='block',
        )(x, w_q, w_k, w_v, w_o, ids.T, probs.T)
        return pl.pallas_call(
            dispatch_kernel,
            out_shape=(jax.ShapeDtypeStruct((tok, d), BF16),
                       jax.ShapeDtypeStruct((held, tokens, d), BF16)),
            in_specs=[vmem_spec] * 3,
            out_specs=(any_spec,) * 2,
            scratch_shapes=[pltpu.VMEM((held, tokens, d), BF16), dma((1 + d // WIDE,))],
            compiler_params=pltpu.CompilerParams(vmem_limit_bytes=16_000_000),
            name='dispatch',
        )(pick, gate, h)

    return jax.shard_map(device_step, mesh=mesh,
                         in_specs=(row_spec, P(), P(), P(), P(), row_spec, row_spec),
                         out_specs=(row_spec, buf_spec), check_vma=False)
```

```python
import math
import jax
import jax.numpy as jnp
from jax import lax
from jax.experimental import pallas as pl
from jax.experimental.pallas import tpu as pltpu
from jax.sharding import PartitionSpec as P

MESH = pl.DeviceIdType.MESH
HEAD = 128
SCALE = 1.0 / math.sqrt(HEAD)
EXP_SCALE = math.log2(math.e) * SCALE
MASKED = -1e30 / SCALE
KC = 1024
NC = 512
RING = 3
WO_BUFS = 4
RED = (80, 64)
EARLY = 2
LAG = 4
FIRST = 2
KV_STEP = 3
WIDE = 512
BLOCK_VMEM = 59_000_000
OUT_SPACE = pltpu.VMEM
F32 = jnp.float32
BF16 = jnp.bfloat16


def block_kernel(x_ref, wq_ref, wk_ref, wv_ref, wo_ref, ids_ref, probs_ref,
                 h_ref, pick_ref, gate_ref,
                 xb, ring, wob, acc, kvacc, kv, ob, oacc, idsb, probsb, tabs,
                 ring_sem, wo_sem, loc_sem, xp_sem, xc_send, xc_recv, xr_send, xr_recv,
                 kv_sem, o_sem, hp_sem, hc_send, hc_recv, hr_sem, t_sem):
    tok, d = x_ref.shape
    own = 2 * tok
    half = wq_ref.shape[1] // 2
    kvw = wk_ref.shape[1] // 2
    nk = d // KC
    per = half // (2 * kvw)
    n_kv = nk // per
    n_loads = n_kv + nk
    oh = d // 2
    nn = oh // NC
    groups = kvw // HEAD
    q_per = half // kvw
    gw = q_per * HEAD
    slots = [(n_loads - RING + i) % RING for i in range(2)]
    units = [(n * NC, NC, n) for n in range(WO_BUFS)]
    units += [((WO_BUFS + i) * NC, NC, slots[i]) for i in range(nn - WO_BUFS)]
    nu = len(units)

    sp = lax.axis_index('sp')
    chip = sp // 2
    core = sp % 2
    partner = chip * 2 + (1 - core)
    across = (1 - chip) * 2 + core
    diag = (1 - chip) * 2 + (1 - core)

    def remote(src, dst, send, recv, dev):
        return pltpu.make_async_remote_copy(
            src_ref=src, dst_ref=dst, send_sem=send, recv_sem=recv,
            device_id={'sp': dev}, device_id_type=MESH)

    def load_kv(n):
        for j in range(per):
            r = pl.ds((n * per + j) * KC, KC)
            c = pl.ds(pl.multiple_of(core * kvw, HEAD), kvw)
            pltpu.make_async_copy(wk_ref.at[r, c], ring.at[n, :, pl.ds(2 * j * kvw, kvw)], ring_sem.at[n]).start()
            pltpu.make_async_copy(wv_ref.at[r, c], ring.at[n, :, pl.ds((2 * j + 1) * kvw, kvw)], ring_sem.at[n]).start()

    def load_q(n):
        slot = n % RING
        r = pl.ds(pl.multiple_of((n - n_kv) * KC, KC), KC)
        c = pl.ds(pl.multiple_of(core * half, HEAD), half)
        pltpu.make_async_copy(wq_ref.at[r, c], ring.at[slot], ring_sem.at[slot]).start()

    def wait_ring(slot):
        pltpu.make_async_copy(wq_ref.at[pl.ds(0, KC), pl.ds(0, half)], ring.at[slot], ring_sem.at[slot]).wait()

    def wo_part(u, j):
        width, slot = units[u][1:]
        return slot, pl.ds(j * width, width)

    def wo_sem_of(u):
        return wo_sem.at[u] if u < WO_BUFS else ring_sem.at[units[u][2]]

    def load_wo(u):
        first, width, slot = units[u]
        c = pl.ds(pl.multiple_of(core * oh + first, HEAD), width)
        step = half if u < WO_BUFS else KC
        for j in range(2 * half // step):
            side = core if j * step < half else 1 - core
            r = pl.ds(pl.multiple_of(side * half + j * step % half, HEAD), step)
            if u < WO_BUFS:
                dst = wob.at[slot, pl.ds(j * step, step), :]
            else:
                dst = ring.at[slot, :, wo_part(u, j)[1]]
            pltpu.make_async_copy(wo_ref.at[r, c], dst, wo_sem_of(u)).start()

    def wait_wo(u):
        width, slot = units[u][1:]
        if u < WO_BUFS:
            copy = pltpu.make_async_copy(wo_ref.at[:, pl.ds(0, NC)], wob.at[slot], wo_sem_of(u))
        else:
            n = half * width // NC
            copy = pltpu.make_async_copy(wq_ref.at[pl.ds(0, KC), pl.ds(0, n)], ring.at[slot, :, pl.ds(0, n)], wo_sem_of(u))
        with jax.named_scope('wwo'):
            copy.wait()

    def times_wo(rows, u):
        slot = units[u][2]
        if u < WO_BUFS:
            return jnp.dot(ob[0:rows, :], wob[slot], preferred_element_type=F32)
        w = jnp.concatenate([ring[slot, :, wo_part(u, j)[1]] for j in range(2 * half // KC)], axis=0)
        return jnp.dot(ob[0:rows, :], w, preferred_element_type=F32)

    barrier = pltpu.get_barrier_semaphore()
    for dev in (partner, across, diag):
        pl.semaphore_signal(barrier, inc=1, device_id={'sp': dev}, device_id_type=MESH)

    own_rows = pl.ds(pl.multiple_of(core * tok, 16), tok)
    x_load = pltpu.make_async_copy(x_ref, xb.at[own_rows, :], loc_sem.at[0])
    ids_load = pltpu.make_async_copy(ids_ref, idsb, loc_sem.at[1])
    probs_load = pltpu.make_async_copy(probs_ref, probsb, loc_sem.at[2])
    x_load.start()
    ids_load.start()
    probs_load.start()
    load_kv(0)

    with jax.named_scope('bar'):
        pl.semaphore_wait(barrier, 3)

    x_pair = remote(x_ref, xb.at[own_rows, :], xp_sem.at[0], xp_sem.at[1], partner)
    x_pair.start()

    def share(c, k):
        return min(RED[c], tok) if k == 0 else max(RED[c] - tok, 0)

    def x_cross(c, k, j):
        n = share(c, k)
        cols = pl.ds(pl.multiple_of(j * KC, KC), KC)
        return remote(x_ref.at[pl.ds(0, n), cols], xb.at[pl.ds(own + k * tok, n), cols], xc_send, xc_recv.at[j], across)

    def x_relay(c, k, j):
        cols = pl.ds(pl.multiple_of(j * KC, KC), KC)
        part = xb.at[pl.ds(own + k * tok, share(c, k)), cols]
        return remote(part, part, xr_send, xr_recv.at[j], partner)

    for c in range(2):
        for k in range(2):
            if share(1 - c, k):
                @pl.when(jnp.logical_and(chip == c, core == k))
                def _():
                    for j in range(nk if k == 0 else FIRST):
                        x_cross(1 - c, k, j).start()

    with jax.named_scope('xl'):
        x_load.wait()
    for n in range(1, RING):
        if n < n_kv:
            load_kv(n)
        else:
            load_q(n)

    ids_load.wait()
    probs_load.wait()
    experts = probsb.shape[0]
    line = lax.broadcasted_iota(jnp.int32, (experts, tok), 0)
    pr = probsb[...]
    hit0 = line == idsb[0:1, :]
    hit1 = line == idsb[1:2, :]
    p0 = jnp.sum(jnp.where(hit0, pr, 0.0), axis=0, keepdims=True)
    p1 = jnp.sum(jnp.where(hit1, pr, 0.0), axis=0, keepdims=True)
    hit = jnp.logical_or(hit0, hit1)
    tabs[sp] = jnp.zeros(tabs.shape[1:], F32)
    tabs[sp, 0:experts, 0:tok] = jnp.where(hit, pr / (p0 + p1), 0.0)
    tabs[sp, experts:2 * experts, 0:tok] = jnp.where(hit, 1.0, 0.0)
    mine = tabs.at[sp]
    for dev in (partner, across, diag):
        remote(mine, mine, t_sem.at[0], t_sem.at[1], dev).start()

    acc[...] = jnp.zeros_like(acc)
    kvacc[...] = jnp.zeros_like(kvacc)

    with jax.named_scope('wxp'):
        x_pair.wait()

    @pl.loop(0, n_kv)
    def _(n):
        with jax.named_scope('wkv'):
            wait_ring(n)
        for j in range(per):
            c = pl.ds(pl.multiple_of((n * per + j) * KC, KC), KC)
            kvacc[...] += jnp.dot(xb[0:own, c], ring[n, :, 2 * j * kvw:2 * (j + 1) * kvw],
                                  preferred_element_type=F32)
        load_q(n + RING)

    for c in range(2):
        if share(1 - c, 1):
            @pl.when(jnp.logical_and(chip == c, core == 1))
            def _():
                for j in range(FIRST, nk):
                    x_cross(1 - c, 1, j).start()

    kv[0:own, :] = kvacc[...].astype(BF16)

    def build_picks():
        with jax.named_scope('tab'):
            three = tabs.at[pl.ds(0, 3)]
            remote(three, three, t_sem.at[0], t_sem.at[1], partner).wait()
        lanes = tabs.shape[2]
        tokens = pick_ref.shape[1]
        held = pick_ref.shape[0] // tokens
        before = lax.broadcasted_iota(jnp.int32, (lanes, lanes), 0) < lax.broadcasted_iota(jnp.int32, (lanes, lanes), 1)
        before = jnp.where(before, 1.0, 0.0).astype(BF16)
        dests, gates = [], []
        for j in range(2):
            dest, g = 0.0, 0.0
            for i in range(2):
                s = (chip if j == 0 else 1 - chip) * 2 + i
                hits = tabs[s, experts:2 * experts, :]
                rank = jnp.dot(hits.astype(BF16), before, preferred_element_type=F32)
                at = jnp.where(hits > 0.5, rank + (s * tok + 1).astype(F32), 0.0)
                gs = tabs[s, 0:experts, :]
                dest = dest + (at if i == 0 else pltpu.roll(at, tok, 1))
                g = g + (gs if i == 0 else pltpu.roll(gs, tok, 1))
            dests.append(dest)
            gates.append(g)
        line = lax.broadcasted_iota(jnp.int32, (experts, lanes), 0)
        slot = lax.broadcasted_iota(jnp.int32, (tokens, lanes), 0).astype(F32) + 1.0
        for e in range(held):
            total = jnp.zeros((tokens, 1), F32)
            for j in range(2):
                here = line == sp * held + e
                dest = jnp.sum(jnp.where(here, dests[j], 0.0), axis=0, keepdims=True)
                g = jnp.sum(jnp.where(here, gates[j], 0.0), axis=0, keepdims=True)
                chosen = slot == dest
                pick_ref[e * tokens:(e + 1) * tokens, j * lanes:(j + 1) * lanes] = jnp.where(chosen, 1.0, 0.0).astype(BF16)
                total = total + jnp.sum(jnp.where(chosen, g, 0.0), axis=1, keepdims=True)
            gate_ref[e * tokens:(e + 1) * tokens, :] = jnp.broadcast_to(total, (tokens, lanes))

    def rest(here):
        red = RED[here]
        rows = own + red
        given = RED[1 - here]
        kv_out, kv_in = (own, red) if here == 0 else (given, own)

        def kv_cross(count):
            return remote(kv.at[pl.ds(0, count), :], kv.at[pl.ds(own, count), :], kv_sem.at[0], kv_sem.at[1], across)

        def pass_on(j):
            for k in range(2):
                if share(here, k):
                    @pl.when(core == k)
                    def _():
                        with jax.named_scope('wxc'):
                            x_cross(here, k, j).wait_recv()
                        x_relay(here, k, j).start()

        @pl.when(core == 0)
        def _():
            kv_cross(kv_out).start()

        pass_on(0)

        @pl.loop(0, nk)
        def _(j):
            @pl.when(j + 1 < nk)
            def _():
                pass_on(j + 1)

            for k in range(2):
                if share(here, k):
                    @pl.when(core == 1 - k)
                    def _():
                        with jax.named_scope('wxr'):
                            x_relay(here, k, j).wait_recv()

            @pl.when(jnp.logical_and(core == 1, j == KV_STEP))
            def _():
                kv_cross(kv_out).start()

            n = n_kv + j
            slot = n % RING
            with jax.named_scope('wq'):
                wait_ring(slot)

            for i in range(2):
                @pl.when(j == nk - 2 + i)
                def _():
                    load_wo(i)

            c = pl.ds(pl.multiple_of(j * KC, KC), KC)
            acc[0:rows, :] += jnp.dot(xb[0:rows, c], ring[slot], preferred_element_type=F32)

            @pl.when(n + RING < n_loads)
            def _():
                load_q(n + RING)

        def o_pair(i):
            first, count = ((0, groups - 1), (groups - 1, 1))[i]
            return remote(ob.at[pl.ds(0, rows), pl.ds(first * gw, count * gw)],
                          ob.at[pl.ds(0, rows), pl.ds(half + first * gw, count * gw)],
                          o_sem.at[2 * i], o_sem.at[2 * i + 1], partner)

        def attend(r0, r1, g, first, last, tri):
            n = r1 - r0
            cols = [slice(g * gw + m * HEAD, g * gw + (m + 1) * HEAD) for m in range(q_per)]
            q = jnp.concatenate([acc[r0:r1, c].astype(BF16) for c in cols], axis=0)
            s = lax.dot_general(q, kv[first:last, g * HEAD:(g + 1) * HEAD], (((1,), (1,)), ((), ())),
                                preferred_element_type=F32)
            lo, hi = tri - first, tri - first + n
            seen = lax.broadcasted_iota(jnp.int32, (n, n), 1) <= lax.broadcasted_iota(jnp.int32, (n, n), 0)
            seen = jnp.concatenate([jnp.where(seen, 1.0, 0.0)] * q_per, axis=0) > 0.5
            parts = [s[:, :lo]] * (lo > 0) + [jnp.where(seen, s[:, lo:hi], MASKED)] + [s[:, hi:]] * (hi < last - first)
            s = jnp.concatenate(parts, axis=1)
            top = jnp.max(s, axis=1, keepdims=True)
            e = jnp.exp2((s - top) * EXP_SCALE)
            w = (e * (1.0 / jnp.sum(e, axis=1, keepdims=True))).astype(BF16)
            o = jnp.dot(w, kv[first:last, kvw + g * HEAD:kvw + (g + 1) * HEAD], preferred_element_type=F32).astype(BF16)
            for m, c in enumerate(cols):
                ob[r0:r1, c] = o[m * n:(m + 1) * n, :]

        load_wo(2)
        with jax.named_scope('wkvx'):
            kv_cross(kv_in).wait_recv()
        for g in range(groups):
            attend(0, own, g, 0, own if here == 0 else 2 * own, 0)
            attend(own, rows, g, 0 if here == 0 else own, rows, own)
            if g == groups - 2:
                with jax.named_scope('os'):
                    o_pair(0).start()
        with jax.named_scope('os'):
            o_pair(1).start()

        def h_cols(u):
            return pl.ds(pl.multiple_of(core * oh + units[u][0], HEAD), units[u][1])

        def h_pair(u):
            part = h_ref.at[pl.ds(0, rows), h_cols(u)]
            return remote(part, part, hp_sem.at[0], hp_sem.at[1], partner)

        def h_send(u):
            return remote(h_ref.at[pl.ds(given, own - given), h_cols(u)],
                          h_ref.at[pl.ds(own + given, own - given), h_cols(u)], hc_send, hc_recv.at[u], across)

        def relay(u):
            part = h_ref.at[pl.ds(rows, own - red), h_cols(u)]
            with jax.named_scope('whc'):
                remote(part, part, hc_send, hc_recv.at[u], across).wait_recv()
            remote(part, part, hr_sem.at[0], hr_sem.at[1], partner).start()

        def finish(u, total):
            h_ref[0:rows, h_cols(u)] = (xb[0:rows, h_cols(u)].astype(F32) + total).astype(BF16)
            h_send(u).start()
            h_pair(u).start()

        load_wo(3)
        for u in range(EARLY):
            wait_wo(u)
            oacc[u, 0:rows, :] = jnp.dot(ob[0:rows, 0:half], wob[u, 0:half, :], preferred_element_type=F32)
        load_wo(nu - 2)
        with jax.named_scope('wo'):
            o_pair(0).wait()
            o_pair(1).wait()
        for u in range(EARLY):
            finish(u, oacc[u, 0:rows, :] + jnp.dot(ob[0:rows, half:2 * half], wob[u, half:2 * half, :],
                                                   preferred_element_type=F32))
            if u == 0:
                load_wo(nu - 1)

        for u in range(EARLY, nu):
            wait_wo(u)
            finish(u, times_wo(rows, u))
            if u >= LAG:
                relay(u - LAG)
        build_picks()
        for u in range(nu - LAG, nu):
            relay(u)

        for k in range(2):
            if share(1 - here, k):
                @pl.when(core == k)
                def _():
                    n = share(1 - here, k)
                    part = xb.at[pl.ds(own + k * tok, n), :]
                    remote(x_ref.at[pl.ds(0, n), :], part, xc_send, xc_recv.at[0], across).wait_send()
            if share(here, k):
                @pl.when(core == k)
                def _():
                    part = xb.at[pl.ds(own + k * tok, share(here, k)), :]
                    remote(part, part, xr_send, xr_recv.at[0], partner).wait_send()
        kv_cross(kv_out).wait_send()

        with jax.named_scope('end'):
            sent = h_ref.at[pl.ds(given, own - given), pl.ds(0, oh)]
            shared = h_ref.at[pl.ds(0, rows), pl.ds(0, oh)]
            late = h_ref.at[pl.ds(rows, own - red), pl.ds(0, oh)]
            remote(sent, sent, hc_send, hc_recv.at[0], across).wait_send()
            remote(shared, shared, hp_sem.at[0], hp_sem.at[1], partner).wait()
            remote(late, late, hr_sem.at[0], hr_sem.at[1], partner).wait()

    for c in range(2):
        pl.when(chip == c)(lambda: rest(c))


def dispatch_kernel(pick_ref, gate_ref, h_ref, hid_ref, buf_ref, out, sems):
    tok, d = hid_ref.shape
    held, tokens = buf_ref.shape[0], buf_ref.shape[1]
    core = lax.axis_index('sp') % 2
    own_rows = pl.ds(pl.multiple_of(core * tok, 16), tok)
    copies = [pltpu.make_async_copy(h_ref.at[own_rows, :], hid_ref, sems.at[0])]
    copies[0].start()
    for i in range(d // WIDE):
        c = slice(i * WIDE, (i + 1) * WIDE)
        y = jnp.dot(pick_ref[...], h_ref[:, c], preferred_element_type=F32)
        for e in range(held):
            r = slice(e * tokens, (e + 1) * tokens)
            g = gate_ref[r, :]
            for j in range(0, WIDE, HEAD):
                out[e, :, i * WIDE + j:i * WIDE + j + HEAD] = (g * y[r, j:j + HEAD]).astype(BF16)
        part = pl.ds(i * WIDE, WIDE)
        copy = pltpu.make_async_copy(out.at[:, :, part], buf_ref.at[:, :, part], sems.at[1 + i])
        copy.start()
        copies.append(copy)
    for copy in copies:
        copy.wait()


def solution(mesh):
    row_spec = P(('dp', 'sp'), None)
    buf_spec = P(('dp', 'sp'), None, None)
    group = mesh.shape['sp']

    def device_step(x, w_q, w_k, w_v, w_o, ids, probs):
        tok, d = x.shape
        half, kvw, oh = w_q.shape[1] // 2, w_k.shape[1] // 2, d // 2
        experts = probs.shape[1]
        held = experts // group
        own, tokens = 2 * tok, group * tok
        rows = own + max(RED)
        nk, nn = d // KC, oh // NC
        any_spec = pl.BlockSpec(memory_space=pl.ANY)
        vmem_spec = pl.BlockSpec(memory_space=pltpu.VMEM)
        dma = pltpu.SemaphoreType.DMA
        h, pick, gate = pl.pallas_call(
            block_kernel,
            out_shape=(OUT_SPACE((tokens, d), BF16),
                       OUT_SPACE((held * tokens, tokens), BF16),
                       OUT_SPACE((held * tokens, 128), F32)),
            in_specs=[any_spec] * 7,
            out_specs=(vmem_spec,) * 3,
            scratch_shapes=[
                pltpu.VMEM((rows, d), BF16),
                pltpu.VMEM((RING, KC, half), BF16),
                pltpu.VMEM((WO_BUFS, d, NC), BF16),
                pltpu.VMEM((rows, half), F32),
                pltpu.VMEM((own, 2 * kvw), F32),
                pltpu.VMEM((tokens, 2 * kvw), BF16),
                pltpu.VMEM((rows, 2 * half), BF16),
                pltpu.VMEM((EARLY, rows, NC), F32),
                pltpu.VMEM((2, tok), jnp.int32),
                pltpu.VMEM((experts, tok), F32),
                pltpu.VMEM((group, 2 * experts, 128), F32),
                dma((RING,)), dma((WO_BUFS,)), dma((3,)), dma((2,)),
                dma(()), dma((nk,)), dma(()), dma((nk,)),
                dma((2,)), dma((4,)), dma((2,)), dma(()), dma((nn,)), dma((2,)), dma((2,)),
            ],
            compiler_params=pltpu.CompilerParams(
                collective_id=0, has_side_effects=True, vmem_limit_bytes=BLOCK_VMEM),
            name='block',
        )(x, w_q, w_k, w_v, w_o, ids.T, probs.T)
        return pl.pallas_call(
            dispatch_kernel,
            out_shape=(jax.ShapeDtypeStruct((tok, d), BF16),
                       jax.ShapeDtypeStruct((held, tokens, d), BF16)),
            in_specs=[vmem_spec] * 3,
            out_specs=(any_spec,) * 2,
            scratch_shapes=[pltpu.VMEM((held, tokens, d), BF16), dma((1 + d // WIDE,))],
            compiler_params=pltpu.CompilerParams(vmem_limit_bytes=16_000_000),
            name='dispatch',
        )(pick, gate, h)

    return jax.shard_map(device_step, mesh=mesh,
                         in_specs=(row_spec, P(), P(), P(), P(), row_spec, row_spec),
                         out_specs=(row_spec, buf_spec), check_vma=False)
```

```python
import math
import jax
import jax.numpy as jnp
from jax import lax
from jax.experimental import pallas as pl
from jax.experimental.pallas import tpu as pltpu
from jax.sharding import PartitionSpec as P

MESH = pl.DeviceIdType.MESH
HEAD = 128
SCALE = 1.0 / math.sqrt(HEAD)
EXP_SCALE = math.log2(math.e) * SCALE
MASKED = -1e30 / SCALE
KC = 1024
NC = 512
RING = 3
WO_BUFS = 4
RED = (80, 64)
EARLY = 2
LAG = 4
FIRST = 2
KV_STEP = 3
WIDE = 512
BLOCK_VMEM = 59_000_000
OUT_SPACE = pltpu.VMEM
F32 = jnp.float32
BF16 = jnp.bfloat16


def block_kernel(x_ref, wq_ref, wk_ref, wv_ref, wo_ref, ids_ref, probs_ref,
                 h_ref, pick_ref, gate_ref,
                 xb, ring, wob, acc, kvacc, kv, ob, oacc, idsb, probsb, tabs,
                 ring_sem, half_sem, wo_sem, loc_sem, xp_sem, xc_send, xc_recv, xr_send, xr_recv,
                 kv_sem, o_sem, hp_sem, hc_send, hc_recv, hr_sem, t_sem):
    tok, d = x_ref.shape
    own = 2 * tok
    half = wq_ref.shape[1] // 2
    kvw = wk_ref.shape[1] // 2
    nk = d // KC
    per = half // (2 * kvw)
    n_kv = nk // per
    n_loads = n_kv + nk
    oh = d // 2
    nn = oh // NC
    groups = kvw // HEAD
    q_per = half // kvw
    gw = q_per * HEAD
    slots = [(n_loads - RING + i) % RING for i in range(2)]
    units = [(n * NC, NC, n) for n in range(WO_BUFS)]
    units += [((WO_BUFS + i) * NC, NC, slots[i]) for i in range(nn - WO_BUFS)]
    nu = len(units)

    sp = lax.axis_index('sp')
    chip = sp // 2
    core = sp % 2
    partner = chip * 2 + (1 - core)
    across = (1 - chip) * 2 + core
    diag = (1 - chip) * 2 + (1 - core)

    def remote(src, dst, send, recv, dev):
        return pltpu.make_async_remote_copy(
            src_ref=src, dst_ref=dst, send_sem=send, recv_sem=recv,
            device_id={'sp': dev}, device_id_type=MESH)

    def load_kv(n):
        for j in range(per):
            r = pl.ds((n * per + j) * KC, KC)
            c = pl.ds(pl.multiple_of(core * kvw, HEAD), kvw)
            pltpu.make_async_copy(wk_ref.at[r, c], ring.at[n, :, pl.ds(2 * j * kvw, kvw)], ring_sem.at[n]).start()
            pltpu.make_async_copy(wv_ref.at[r, c], ring.at[n, :, pl.ds((2 * j + 1) * kvw, kvw)], ring_sem.at[n]).start()

    def load_q(n):
        slot = n % RING
        r = pl.ds(pl.multiple_of((n - n_kv) * KC, KC), KC)
        c = pl.ds(pl.multiple_of(core * half, HEAD), half)
        pltpu.make_async_copy(wq_ref.at[r, c], ring.at[slot], ring_sem.at[slot]).start()

    def load_q_last():
        slot = (n_loads - 1) % RING
        c = pl.ds(pl.multiple_of(core * half, HEAD), half)
        for i in range(2):
            r = pl.ds(d - KC + i * KC // 2, KC // 2)
            pltpu.make_async_copy(wq_ref.at[r, c], ring.at[slot, pl.ds(i * KC // 2, KC // 2), :], half_sem.at[i]).start()

    def wait_half(slot, i):
        r = pl.ds(i * KC // 2, KC // 2)
        pltpu.make_async_copy(wq_ref.at[r, pl.ds(0, half)], ring.at[slot, r, :], half_sem.at[i]).wait()

    def wait_ring(slot):
        pltpu.make_async_copy(wq_ref.at[pl.ds(0, KC), pl.ds(0, half)], ring.at[slot], ring_sem.at[slot]).wait()

    def wo_part(u, j):
        width, slot = units[u][1:]
        return slot, pl.ds(j * width, width)

    def wo_sem_of(u):
        return wo_sem.at[u] if u < WO_BUFS else ring_sem.at[units[u][2]]

    def wo_copy_sem(u, j):
        return half_sem.at[j * KC // half] if u == nu - 1 else wo_sem_of(u)

    def load_wo(u):
        first, width, slot = units[u]
        c = pl.ds(pl.multiple_of(core * oh + first, HEAD), width)
        step = half if u < WO_BUFS else KC
        for j in range(2 * half // step):
            side = core if j * step < half else 1 - core
            r = pl.ds(pl.multiple_of(side * half + j * step % half, HEAD), step)
            if u < WO_BUFS:
                dst = wob.at[slot, pl.ds(j * step, step), :]
            else:
                dst = ring.at[slot, :, wo_part(u, j)[1]]
            pltpu.make_async_copy(wo_ref.at[r, c], dst, wo_copy_sem(u, j)).start()

    def wait_wo(u):
        width, slot = units[u][1:]
        if u < WO_BUFS:
            copy = pltpu.make_async_copy(wo_ref.at[:, pl.ds(0, NC)], wob.at[slot], wo_sem_of(u))
        else:
            n = half * width // NC
            copy = pltpu.make_async_copy(wq_ref.at[pl.ds(0, KC), pl.ds(0, n)], ring.at[slot, :, pl.ds(0, n)], wo_sem_of(u))
        with jax.named_scope('wwo'):
            copy.wait()

    def times_wo(o, u, first=0, last=2 * half):
        slot = units[u][2]
        if u < WO_BUFS:
            w = wob[slot, first:last, :]
        else:
            w = jnp.concatenate([ring[slot, :, wo_part(u, j)[1]] for j in range(first // KC, last // KC)], axis=0)
        return jnp.dot(o, w, preferred_element_type=F32)

    barrier = pltpu.get_barrier_semaphore()
    for dev in (partner, across, diag):
        pl.semaphore_signal(barrier, inc=1, device_id={'sp': dev}, device_id_type=MESH)

    own_rows = pl.ds(pl.multiple_of(core * tok, 16), tok)
    x_load = pltpu.make_async_copy(x_ref, xb.at[own_rows, :], loc_sem.at[0])
    ids_load = pltpu.make_async_copy(ids_ref, idsb, loc_sem.at[1])
    probs_load = pltpu.make_async_copy(probs_ref, probsb, loc_sem.at[2])
    x_load.start()
    ids_load.start()
    probs_load.start()
    load_kv(0)

    with jax.named_scope('bar'):
        pl.semaphore_wait(barrier, 3)

    x_pair = remote(x_ref, xb.at[own_rows, :], xp_sem.at[0], xp_sem.at[1], partner)
    x_pair.start()

    def share(c, k):
        return min(RED[c], tok) if k == 0 else max(RED[c] - tok, 0)

    def x_cross(c, k, j, early=False):
        n = share(c, k)
        cols = pl.ds(pl.multiple_of(j * KC, KC), KC)
        return remote(x_ref.at[pl.ds(0, n), cols] if early else xb.at[pl.ds(k * tok, n), cols], xb.at[pl.ds(own + k * tok, n), cols], xc_send, xc_recv.at[j], across)

    def x_relay(c, k, j):
        cols = pl.ds(pl.multiple_of(j * KC, KC), KC)
        part = xb.at[pl.ds(own + k * tok, share(c, k)), cols]
        return remote(part, part, xr_send, xr_recv.at[j], partner)

    for c in range(2):
        for k in range(2):
            if share(1 - c, k):
                @pl.when(jnp.logical_and(chip == c, core == k))
                def _():
                    for j in range(FIRST):
                        x_cross(1 - c, k, j, early=True).start()

    with jax.named_scope('xl'):
        x_load.wait()
    for c in range(2):
        @pl.when(jnp.logical_and(chip == c, core == 0))
        def _():
            for j in range(FIRST, nk):
                x_cross(1 - c, 0, j).start()
    for n in range(1, RING):
        if n < n_kv:
            load_kv(n)
        else:
            load_q(n)

    ids_load.wait()
    probs_load.wait()
    experts = probsb.shape[0]
    line = lax.broadcasted_iota(jnp.int32, (experts, tok), 0)
    pr = probsb[...]
    hit0 = line == idsb[0:1, :]
    hit1 = line == idsb[1:2, :]
    p0 = jnp.sum(jnp.where(hit0, pr, 0.0), axis=0, keepdims=True)
    p1 = jnp.sum(jnp.where(hit1, pr, 0.0), axis=0, keepdims=True)
    hit = jnp.logical_or(hit0, hit1)
    tabs[sp] = jnp.zeros(tabs.shape[1:], F32)
    tabs[sp, 0:experts, 0:tok] = jnp.where(hit, pr / (p0 + p1), 0.0)
    tabs[sp, experts:2 * experts, 0:tok] = jnp.where(hit, 1.0, 0.0)
    mine = tabs.at[sp]
    for dev in (partner, across, diag):
        remote(mine, mine, t_sem.at[0], t_sem.at[1], dev).start()

    acc[...] = jnp.zeros_like(acc)
    kvacc[...] = jnp.zeros_like(kvacc)

    with jax.named_scope('wxp'):
        x_pair.wait()

    @pl.loop(0, n_kv)
    def _(n):
        with jax.named_scope('wkv'):
            wait_ring(n)
        for j in range(per):
            c = pl.ds(pl.multiple_of((n * per + j) * KC, KC), KC)
            kvacc[...] += jnp.dot(xb[0:own, c], ring[n, :, 2 * j * kvw:2 * (j + 1) * kvw],
                                  preferred_element_type=F32)
        load_q(n + RING)

    for c in range(2):
        if share(1 - c, 1):
            @pl.when(jnp.logical_and(chip == c, core == 1))
            def _():
                for j in range(FIRST, nk):
                    x_cross(1 - c, 1, j).start()

    kv[0:own, :] = kvacc[...].astype(BF16)

    def build_picks():
        with jax.named_scope('tab'):
            three = tabs.at[pl.ds(0, 3)]
            remote(three, three, t_sem.at[0], t_sem.at[1], partner).wait()
        lanes = tabs.shape[2]
        tokens = pick_ref.shape[1]
        held = pick_ref.shape[0] // tokens
        before = lax.broadcasted_iota(jnp.int32, (lanes, lanes), 0) < lax.broadcasted_iota(jnp.int32, (lanes, lanes), 1)
        before = jnp.where(before, 1.0, 0.0).astype(BF16)
        dests, gates = [], []
        for j in range(2):
            dest, g = 0.0, 0.0
            for i in range(2):
                s = (chip if j == 0 else 1 - chip) * 2 + i
                hits = tabs[s, experts:2 * experts, :]
                rank = jnp.dot(hits.astype(BF16), before, preferred_element_type=F32)
                at = jnp.where(hits > 0.5, rank + (s * tok + 1).astype(F32), 0.0)
                gs = tabs[s, 0:experts, :]
                dest = dest + (at if i == 0 else pltpu.roll(at, tok, 1))
                g = g + (gs if i == 0 else pltpu.roll(gs, tok, 1))
            dests.append(dest)
            gates.append(g)
        line = lax.broadcasted_iota(jnp.int32, (experts, lanes), 0)
        slot = lax.broadcasted_iota(jnp.int32, (tokens, lanes), 0).astype(F32) + 1.0
        for e in range(held):
            total = jnp.zeros((tokens, 1), F32)
            for j in range(2):
                here = line == sp * held + e
                dest = jnp.sum(jnp.where(here, dests[j], 0.0), axis=0, keepdims=True)
                g = jnp.sum(jnp.where(here, gates[j], 0.0), axis=0, keepdims=True)
                chosen = slot == dest
                pick_ref[e * tokens:(e + 1) * tokens, j * lanes:(j + 1) * lanes] = jnp.where(chosen, 1.0, 0.0).astype(BF16)
                total = total + jnp.sum(jnp.where(chosen, g, 0.0), axis=1, keepdims=True)
            gate_ref[e * tokens:(e + 1) * tokens, :] = jnp.broadcast_to(total, (tokens, lanes))

    def rest(here):
        red = RED[here]
        rows = own + red
        given = RED[1 - here]
        kv_out, kv_in = (own, red) if here == 0 else (given, own)

        def kv_cross(count):
            return remote(kv.at[pl.ds(0, count), :], kv.at[pl.ds(own, count), :], kv_sem.at[0], kv_sem.at[1], across)

        def pass_on(j):
            for k in range(2):
                if share(here, k):
                    @pl.when(core == k)
                    def _():
                        with jax.named_scope('wxc'):
                            x_cross(here, k, j).wait_recv()
                        x_relay(here, k, j).start()

        @pl.when(core == 0)
        def _():
            kv_cross(kv_out).start()

        pass_on(0)

        def take_relay(j):
            for k in range(2):
                if share(here, k):
                    @pl.when(core == 1 - k)
                    def _():
                        with jax.named_scope('wxr'):
                            x_relay(here, k, j).wait_recv()

        @pl.loop(0, nk - 1)
        def _(j):
            pass_on(j + 1)
            take_relay(j)

            @pl.when(jnp.logical_and(core == 1, j == KV_STEP))
            def _():
                kv_cross(kv_out).start()

            n = n_kv + j
            slot = n % RING
            with jax.named_scope('wq'):
                wait_ring(slot)

            @pl.when(j == nk - 2)
            def _():
                load_wo(0)

            c = pl.ds(pl.multiple_of(j * KC, KC), KC)
            acc[0:rows, :] += jnp.dot(xb[0:rows, c], ring[slot], preferred_element_type=F32)

            @pl.when(n + RING < n_loads - 1)
            def _():
                load_q(n + RING)

            @pl.when(n + RING == n_loads - 1)
            def _():
                load_q_last()

        take_relay(nk - 1)
        slot = (n_loads - 1) % RING
        for i in range(2):
            with jax.named_scope('wqh'):
                wait_half(slot, i)
            if i == 0:
                load_wo(1)
            r = slice(i * KC // 2, (i + 1) * KC // 2)
            acc[0:rows, :] += jnp.dot(xb[0:rows, d - KC + r.start:d - KC + r.stop], ring[slot, r, :],
                                      preferred_element_type=F32)

        def o_pair(i):
            first, count = ((0, groups - 1), (groups - 1, 1))[i]
            return remote(ob.at[pl.ds(0, rows), pl.ds(first * gw, count * gw)],
                          ob.at[pl.ds(0, rows), pl.ds(half + first * gw, count * gw)],
                          o_sem.at[2 * i], o_sem.at[2 * i + 1], partner)

        def attend(r0, r1, g, first, last, tri):
            n = r1 - r0
            cols = [slice(g * gw + m * HEAD, g * gw + (m + 1) * HEAD) for m in range(q_per)]
            q = jnp.concatenate([acc[r0:r1, c].astype(BF16) for c in cols], axis=0)
            s = lax.dot_general(q, kv[first:last, g * HEAD:(g + 1) * HEAD], (((1,), (1,)), ((), ())),
                                preferred_element_type=F32)
            lo, hi = tri - first, tri - first + n
            seen = lax.broadcasted_iota(jnp.int32, (n, n), 1) <= lax.broadcasted_iota(jnp.int32, (n, n), 0)
            seen = jnp.concatenate([jnp.where(seen, 1.0, 0.0)] * q_per, axis=0) > 0.5
            parts = [s[:, :lo]] * (lo > 0) + [jnp.where(seen, s[:, lo:hi], MASKED)] + [s[:, hi:]] * (hi < last - first)
            s = jnp.concatenate(parts, axis=1)
            top = jnp.max(s, axis=1, keepdims=True)
            e = jnp.exp2((s - top) * EXP_SCALE)
            w = (e * (1.0 / jnp.sum(e, axis=1, keepdims=True))).astype(BF16)
            o = jnp.dot(w, kv[first:last, kvw + g * HEAD:kvw + (g + 1) * HEAD], preferred_element_type=F32).astype(BF16)
            for m, c in enumerate(cols):
                ob[r0:r1, c] = o[m * n:(m + 1) * n, :]

        load_wo(2)
        with jax.named_scope('wkvx'):
            kv_cross(kv_in).wait_recv()
        for g in range(groups):
            attend(0, own, g, 0, own if here == 0 else 2 * own, 0)
            attend(own, rows, g, 0 if here == 0 else own, rows, own)
            if g == groups - 2:
                with jax.named_scope('os'):
                    o_pair(0).start()
        with jax.named_scope('os'):
            o_pair(1).start()

        def h_cols(u):
            return pl.ds(pl.multiple_of(core * oh + units[u][0], HEAD), units[u][1])

        def h_pair(u):
            part = h_ref.at[pl.ds(0, rows), h_cols(u)]
            return remote(part, part, hp_sem.at[0], hp_sem.at[1], partner)

        def h_send(u):
            return remote(h_ref.at[pl.ds(given, own - given), h_cols(u)],
                          h_ref.at[pl.ds(own + given, own - given), h_cols(u)], hc_send, hc_recv.at[u], across)

        def relay(u):
            part = h_ref.at[pl.ds(rows, own - red), h_cols(u)]
            with jax.named_scope('whc'):
                remote(part, part, hc_send, hc_recv.at[u], across).wait_recv()
            remote(part, part, hr_sem.at[0], hr_sem.at[1], partner).start()

        def put(first, last, u, total):
            h_ref[first:last, h_cols(u)] = (xb[first:last, h_cols(u)].astype(F32) + total).astype(BF16)

        def finish(u, total):
            put(0, rows, u, total)
            h_send(u).start()
            h_pair(u).start()

        load_wo(3)
        for u in range(EARLY):
            wait_wo(u)
            oacc[u, 0:rows, :] = jnp.dot(ob[0:rows, 0:half], wob[u, 0:half, :], preferred_element_type=F32)
        load_wo(nu - 2)
        with jax.named_scope('wo'):
            o_pair(0).wait()
            o_pair(1).wait()
        for u in range(EARLY):
            finish(u, oacc[u, 0:rows, :] + jnp.dot(ob[0:rows, half:2 * half], wob[u, half:2 * half, :],
                                                   preferred_element_type=F32))
            if u == 0:
                load_wo(nu - 1)

        for u in range(EARLY, nu):
            if u < nu - 1:
                wait_wo(u)
                finish(u, times_wo(ob[0:rows, :], u))
            else:
                first, last = (0, rows) if here == 0 else (given, own)
                wait_half(units[u][2], 0)
                oacc[0, first:last, :] = times_wo(ob[first:last, 0:half], u, 0, half)
                with jax.named_scope('wwh'):
                    wait_half(units[u][2], 1)
                put(first, last, u, oacc[0, first:last, :] + times_wo(ob[first:last, half:2 * half], u, half, 2 * half))
                h_send(u).start()
                if here == 1:
                    o = jnp.concatenate([ob[0:given, :], ob[own:rows, :]], axis=0)
                    total = times_wo(o, u)
                    put(0, given, u, total[0:given])
                    put(own, rows, u, total[given:])
                h_pair(u).start()
            if u >= LAG:
                relay(u - LAG)
        build_picks()
        for u in range(nu - LAG, nu):
            relay(u)

        for k in range(2):
            if share(1 - here, k):
                @pl.when(core == k)
                def _():
                    n = share(1 - here, k)
                    part = xb.at[pl.ds(own + k * tok, n), :]
                    remote(x_ref.at[pl.ds(0, n), :], part, xc_send, xc_recv.at[0], across).wait_send()
            if share(here, k):
                @pl.when(core == k)
                def _():
                    part = xb.at[pl.ds(own + k * tok, share(here, k)), :]
                    remote(part, part, xr_send, xr_recv.at[0], partner).wait_send()
        kv_cross(kv_out).wait_send()

        with jax.named_scope('end'):
            sent = h_ref.at[pl.ds(given, own - given), pl.ds(0, oh)]
            shared = h_ref.at[pl.ds(0, rows), pl.ds(0, oh)]
            late = h_ref.at[pl.ds(rows, own - red), pl.ds(0, oh)]
            remote(sent, sent, hc_send, hc_recv.at[0], across).wait_send()
            remote(shared, shared, hp_sem.at[0], hp_sem.at[1], partner).wait()
            remote(late, late, hr_sem.at[0], hr_sem.at[1], partner).wait()

    for c in range(2):
        pl.when(chip == c)(lambda: rest(c))


def dispatch_kernel(pick_ref, gate_ref, h_ref, hid_ref, buf_ref, out, sems):
    tok, d = hid_ref.shape
    held, tokens = buf_ref.shape[0], buf_ref.shape[1]
    core = lax.axis_index('sp') % 2
    own_rows = pl.ds(pl.multiple_of(core * tok, 16), tok)
    hidden = pltpu.make_async_copy(h_ref.at[own_rows, :], hid_ref, sems.at[0])
    hidden.start()
    for i in range(d // WIDE):
        c = slice(i * WIDE, (i + 1) * WIDE)
        y = jnp.dot(pick_ref[...], h_ref[:, c], preferred_element_type=F32)
        for e in range(held):
            r = slice(e * tokens, (e + 1) * tokens)
            g = gate_ref[r, :]
            for j in range(0, WIDE, HEAD):
                out[e, :, i * WIDE + j:i * WIDE + j + HEAD] = (g * y[r, j:j + HEAD]).astype(BF16)
        part = pl.ds(i * WIDE, WIDE)
        pltpu.make_async_copy(out.at[:, :, part], buf_ref.at[:, :, part], sems.at[1]).start()
    hidden.wait()
    pltpu.make_async_copy(out, buf_ref, sems.at[1]).wait()


def solution(mesh):
    row_spec = P(('dp', 'sp'), None)
    buf_spec = P(('dp', 'sp'), None, None)
    group = mesh.shape['sp']

    def device_step(x, w_q, w_k, w_v, w_o, ids, probs):
        tok, d = x.shape
        half, kvw, oh = w_q.shape[1] // 2, w_k.shape[1] // 2, d // 2
        experts = probs.shape[1]
        held = experts // group
        own, tokens = 2 * tok, group * tok
        rows = own + max(RED)
        nk, nn = d // KC, oh // NC
        any_spec = pl.BlockSpec(memory_space=pl.ANY)
        vmem_spec = pl.BlockSpec(memory_space=pltpu.VMEM)
        dma = pltpu.SemaphoreType.DMA
        h, pick, gate = pl.pallas_call(
            block_kernel,
            out_shape=(OUT_SPACE((tokens, d), BF16),
                       OUT_SPACE((held * tokens, tokens), BF16),
                       OUT_SPACE((held * tokens, 128), F32)),
            in_specs=[any_spec] * 7,
            out_specs=(vmem_spec,) * 3,
            scratch_shapes=[
                pltpu.VMEM((rows, d), BF16),
                pltpu.VMEM((RING, KC, half), BF16),
                pltpu.VMEM((WO_BUFS, d, NC), BF16),
                pltpu.VMEM((rows, half), F32),
                pltpu.VMEM((own, 2 * kvw), F32),
                pltpu.VMEM((tokens, 2 * kvw), BF16),
                pltpu.VMEM((rows, 2 * half), BF16),
                pltpu.VMEM((EARLY, rows, NC), F32),
                pltpu.VMEM((2, tok), jnp.int32),
                pltpu.VMEM((experts, tok), F32),
                pltpu.VMEM((group, 2 * experts, 128), F32),
                dma((RING,)), dma((2,)), dma((WO_BUFS,)), dma((3,)), dma((2,)),
                dma(()), dma((nk,)), dma(()), dma((nk,)),
                dma((2,)), dma((4,)), dma((2,)), dma(()), dma((nn,)), dma((2,)), dma((2,)),
            ],
            compiler_params=pltpu.CompilerParams(
                collective_id=0, has_side_effects=True, vmem_limit_bytes=BLOCK_VMEM),
            name='block',
        )(x, w_q, w_k, w_v, w_o, ids.T, probs.T)
        return pl.pallas_call(
            dispatch_kernel,
            out_shape=(jax.ShapeDtypeStruct((tok, d), BF16),
                       jax.ShapeDtypeStruct((held, tokens, d), BF16)),
            in_specs=[vmem_spec] * 3,
            out_specs=(any_spec,) * 2,
            scratch_shapes=[pltpu.VMEM((held, tokens, d), BF16), dma((2,))],
            compiler_params=pltpu.CompilerParams(vmem_limit_bytes=16_000_000),
            name='dispatch',
        )(pick, gate, h)

    return jax.shard_map(device_step, mesh=mesh,
                         in_specs=(row_spec, P(), P(), P(), P(), row_spec, row_spec),
                         out_specs=(row_spec, buf_spec), check_vma=False)
```

```python
import math
import jax
import jax.numpy as jnp
from jax import lax
from jax.experimental import pallas as pl
from jax.experimental.pallas import tpu as pltpu
from jax.sharding import PartitionSpec as P

MESH = pl.DeviceIdType.MESH
HEAD = 128
SCALE = 1.0 / math.sqrt(HEAD)
EXP_SCALE = math.log2(math.e) * SCALE
MASKED = -1e30 / SCALE
KC = 1024
NC = 512
RING = 3
WO_BUFS = 4
RED = (80, 64)
EARLY = 2
LAG = 4
FIRST = 2
KV_STEP = 3
WIDE = 512
BLOCK_VMEM = 59_000_000
OUT_SPACE = pltpu.VMEM
F32 = jnp.float32
BF16 = jnp.bfloat16


def block_kernel(x_ref, wq_ref, wk_ref, wv_ref, wo_ref, ids_ref, probs_ref,
                 h_ref, pick_ref, gate_ref,
                 xb, ring, wob, acc, kvacc, kv, ob, oacc, idsb, probsb, tabs,
                 ring_sem, half_sem, wo_sem, loc_sem, xp_sem, xc_send, xc_recv, xr_send, xr_recv,
                 kv_sem, o_sem, hp_sem, hc_send, hc_recv, hr_sem, t_sem):
    tok, d = x_ref.shape
    own = 2 * tok
    half = wq_ref.shape[1] // 2
    kvw = wk_ref.shape[1] // 2
    nk = d // KC
    per = half // (2 * kvw)
    n_kv = nk // per
    n_loads = n_kv + nk
    oh = d // 2
    nn = oh // NC
    groups = kvw // HEAD
    q_per = half // kvw
    gw = q_per * HEAD
    slots = [(n_loads - RING + i) % RING for i in range(2)]
    units = [(n * NC, NC, n) for n in range(WO_BUFS)]
    units += [((WO_BUFS + i) * NC, NC, slots[i]) for i in range(nn - WO_BUFS)]
    nu = len(units)

    sp = lax.axis_index('sp')
    chip = sp // 2
    core = sp % 2
    partner = chip * 2 + (1 - core)
    across = (1 - chip) * 2 + core
    diag = (1 - chip) * 2 + (1 - core)

    def remote(src, dst, send, recv, dev):
        return pltpu.make_async_remote_copy(
            src_ref=src, dst_ref=dst, send_sem=send, recv_sem=recv,
            device_id={'sp': dev}, device_id_type=MESH)

    def load_kv(n):
        for j in range(per):
            r = pl.ds((n * per + j) * KC, KC)
            c = pl.ds(pl.multiple_of(core * kvw, HEAD), kvw)
            pltpu.make_async_copy(wk_ref.at[r, c], ring.at[n, :, pl.ds(2 * j * kvw, kvw)], ring_sem.at[n]).start()
            pltpu.make_async_copy(wv_ref.at[r, c], ring.at[n, :, pl.ds((2 * j + 1) * kvw, kvw)], ring_sem.at[n]).start()

    def load_q(n):
        slot = n % RING
        r = pl.ds(pl.multiple_of((n - n_kv) * KC, KC), KC)
        c = pl.ds(pl.multiple_of(core * half, HEAD), half)
        pltpu.make_async_copy(wq_ref.at[r, c], ring.at[slot], ring_sem.at[slot]).start()

    def load_q_last():
        slot = (n_loads - 1) % RING
        c = pl.ds(pl.multiple_of(core * half, HEAD), half)
        for i in range(2):
            r = pl.ds(d - KC + i * KC // 2, KC // 2)
            pltpu.make_async_copy(wq_ref.at[r, c], ring.at[slot, pl.ds(i * KC // 2, KC // 2), :], half_sem.at[i]).start()

    def wait_half(slot, i):
        r = pl.ds(i * KC // 2, KC // 2)
        pltpu.make_async_copy(wq_ref.at[r, pl.ds(0, half)], ring.at[slot, r, :], half_sem.at[i]).wait()

    def wait_ring(slot):
        pltpu.make_async_copy(wq_ref.at[pl.ds(0, KC), pl.ds(0, half)], ring.at[slot], ring_sem.at[slot]).wait()

    def wo_part(u, j):
        width, slot = units[u][1:]
        return slot, pl.ds(j * width, width)

    def wo_sem_of(u):
        return wo_sem.at[u] if u < WO_BUFS else ring_sem.at[units[u][2]]

    def wo_copy_sem(u, j):
        return half_sem.at[j * KC // half] if u == nu - 1 else wo_sem_of(u)

    def load_wo(u):
        first, width, slot = units[u]
        c = pl.ds(pl.multiple_of(core * oh + first, HEAD), width)
        step = half if u < WO_BUFS else KC
        for j in range(2 * half // step):
            side = core if j * step < half else 1 - core
            r = pl.ds(pl.multiple_of(side * half + j * step % half, HEAD), step)
            if u < WO_BUFS:
                dst = wob.at[slot, pl.ds(j * step, step), :]
            else:
                dst = ring.at[slot, :, wo_part(u, j)[1]]
            pltpu.make_async_copy(wo_ref.at[r, c], dst, wo_copy_sem(u, j)).start()

    def wait_wo(u):
        width, slot = units[u][1:]
        if u < WO_BUFS:
            copy = pltpu.make_async_copy(wo_ref.at[:, pl.ds(0, NC)], wob.at[slot], wo_sem_of(u))
        else:
            n = half * width // NC
            copy = pltpu.make_async_copy(wq_ref.at[pl.ds(0, KC), pl.ds(0, n)], ring.at[slot, :, pl.ds(0, n)], wo_sem_of(u))
        with jax.named_scope('wwo'):
            copy.wait()

    def times_wo(o, u, first=0, last=2 * half):
        slot = units[u][2]
        if u < WO_BUFS:
            w = wob[slot, first:last, :]
        else:
            w = jnp.concatenate([ring[slot, :, wo_part(u, j)[1]] for j in range(first // KC, last // KC)], axis=0)
        return jnp.dot(o, w, preferred_element_type=F32)

    barrier = pltpu.get_barrier_semaphore()
    for dev in (partner, across, diag):
        pl.semaphore_signal(barrier, inc=1, device_id={'sp': dev}, device_id_type=MESH)

    own_rows = pl.ds(pl.multiple_of(core * tok, 16), tok)
    x_load = pltpu.make_async_copy(x_ref, xb.at[own_rows, :], loc_sem.at[0])
    ids_load = pltpu.make_async_copy(ids_ref, idsb, loc_sem.at[1])
    probs_load = pltpu.make_async_copy(probs_ref, probsb, loc_sem.at[2])
    x_load.start()
    ids_load.start()
    probs_load.start()
    load_kv(0)

    with jax.named_scope('bar'):
        pl.semaphore_wait(barrier, 3)

    x_pair = remote(x_ref, xb.at[own_rows, :], xp_sem.at[0], xp_sem.at[1], partner)
    x_pair.start()

    def share(c, k):
        return min(RED[c], tok) if k == 0 else max(RED[c] - tok, 0)

    def x_cross(c, k, j, early=False):
        n = share(c, k)
        cols = pl.ds(pl.multiple_of(j * KC, KC), KC)
        return remote(x_ref.at[pl.ds(0, n), cols] if early else xb.at[pl.ds(k * tok, n), cols], xb.at[pl.ds(own + k * tok, n), cols], xc_send, xc_recv.at[j], across)

    def x_relay(c, k, j):
        cols = pl.ds(pl.multiple_of(j * KC, KC), KC)
        part = xb.at[pl.ds(own + k * tok, share(c, k)), cols]
        return remote(part, part, xr_send, xr_recv.at[j], partner)

    for c in range(2):
        for k in range(2):
            if share(1 - c, k):
                @pl.when(jnp.logical_and(chip == c, core == k))
                def _():
                    for j in range(FIRST):
                        x_cross(1 - c, k, j, early=True).start()

    with jax.named_scope('xl'):
        x_load.wait()
    for c in range(2):
        @pl.when(jnp.logical_and(chip == c, core == 0))
        def _():
            for j in range(FIRST, nk):
                x_cross(1 - c, 0, j).start()
    for n in range(1, RING):
        if n < n_kv:
            load_kv(n)
        else:
            load_q(n)

    ids_load.wait()
    probs_load.wait()
    experts = probsb.shape[0]
    line = lax.broadcasted_iota(jnp.int32, (experts, tok), 0)
    pr = probsb[...]
    hit0 = line == idsb[0:1, :]
    hit1 = line == idsb[1:2, :]
    p0 = jnp.sum(jnp.where(hit0, pr, 0.0), axis=0, keepdims=True)
    p1 = jnp.sum(jnp.where(hit1, pr, 0.0), axis=0, keepdims=True)
    hit = jnp.logical_or(hit0, hit1)
    tabs[sp] = jnp.zeros(tabs.shape[1:], F32)
    tabs[sp, 0:experts, 0:tok] = jnp.where(hit, pr / (p0 + p1), 0.0)
    tabs[sp, experts:2 * experts, 0:tok] = jnp.where(hit, 1.0, 0.0)
    acc[...] = jnp.zeros_like(acc)
    kvacc[...] = jnp.zeros_like(kvacc)

    with jax.named_scope('wxp'):
        x_pair.wait()

    @pl.loop(0, n_kv)
    def _(n):
        with jax.named_scope('wkv'):
            wait_ring(n)
        for j in range(per):
            c = pl.ds(pl.multiple_of((n * per + j) * KC, KC), KC)
            kvacc[...] += jnp.dot(xb[0:own, c], ring[n, :, 2 * j * kvw:2 * (j + 1) * kvw],
                                  preferred_element_type=F32)
        load_q(n + RING)

    for c in range(2):
        if share(1 - c, 1):
            @pl.when(jnp.logical_and(chip == c, core == 1))
            def _():
                for j in range(FIRST, nk):
                    x_cross(1 - c, 1, j).start()

    kv[0:own, :] = kvacc[...].astype(BF16)

    def build_picks():
        with jax.named_scope('tab'):
            three = tabs.at[pl.ds(0, 3)]
            remote(three, three, t_sem.at[0], t_sem.at[1], partner).wait()
        lanes = tabs.shape[2]
        tokens = pick_ref.shape[1]
        held = pick_ref.shape[0] // tokens
        before = lax.broadcasted_iota(jnp.int32, (lanes, lanes), 0) < lax.broadcasted_iota(jnp.int32, (lanes, lanes), 1)
        before = jnp.where(before, 1.0, 0.0).astype(BF16)
        dests, gates = [], []
        for j in range(2):
            dest, g = 0.0, 0.0
            for i in range(2):
                s = (chip if j == 0 else 1 - chip) * 2 + i
                hits = tabs[s, experts:2 * experts, :]
                rank = jnp.dot(hits.astype(BF16), before, preferred_element_type=F32)
                at = jnp.where(hits > 0.5, rank + (s * tok + 1).astype(F32), 0.0)
                gs = tabs[s, 0:experts, :]
                dest = dest + (at if i == 0 else pltpu.roll(at, tok, 1))
                g = g + (gs if i == 0 else pltpu.roll(gs, tok, 1))
            dests.append(dest)
            gates.append(g)
        line = lax.broadcasted_iota(jnp.int32, (experts, lanes), 0)
        slot = lax.broadcasted_iota(jnp.int32, (tokens, lanes), 0).astype(F32) + 1.0
        for e in range(held):
            total = jnp.zeros((tokens, 1), F32)
            for j in range(2):
                here = line == sp * held + e
                dest = jnp.sum(jnp.where(here, dests[j], 0.0), axis=0, keepdims=True)
                g = jnp.sum(jnp.where(here, gates[j], 0.0), axis=0, keepdims=True)
                chosen = slot == dest
                pick_ref[e * tokens:(e + 1) * tokens, j * lanes:(j + 1) * lanes] = jnp.where(chosen, 1.0, 0.0).astype(BF16)
                total = total + jnp.sum(jnp.where(chosen, g, 0.0), axis=1, keepdims=True)
            gate_ref[e * tokens:(e + 1) * tokens, :] = jnp.broadcast_to(total, (tokens, lanes))

    def rest(here):
        red = RED[here]
        rows = own + red
        given = RED[1 - here]
        kv_out, kv_in = (own, red) if here == 0 else (given, own)

        def kv_cross(count):
            return remote(kv.at[pl.ds(0, count), :], kv.at[pl.ds(own, count), :], kv_sem.at[0], kv_sem.at[1], across)

        def pass_on(j):
            for k in range(2):
                if share(here, k):
                    @pl.when(core == k)
                    def _():
                        with jax.named_scope('wxc'):
                            x_cross(here, k, j).wait_recv()
                        x_relay(here, k, j).start()

        @pl.when(core == 0)
        def _():
            kv_cross(kv_out).start()

        pass_on(0)

        def take_relay(j):
            for k in range(2):
                if share(here, k):
                    @pl.when(core == 1 - k)
                    def _():
                        with jax.named_scope('wxr'):
                            x_relay(here, k, j).wait_recv()

        @pl.loop(0, nk - 1)
        def _(j):
            pass_on(j + 1)
            take_relay(j)

            @pl.when(jnp.logical_and(core == 1, j == KV_STEP))
            def _():
                kv_cross(kv_out).start()

            n = n_kv + j
            slot = n % RING
            with jax.named_scope('wq'):
                wait_ring(slot)

            @pl.when(j == nk - 2)
            def _():
                load_wo(0)

            c = pl.ds(pl.multiple_of(j * KC, KC), KC)
            acc[0:rows, :] += jnp.dot(xb[0:rows, c], ring[slot], preferred_element_type=F32)

            @pl.when(n + RING < n_loads - 1)
            def _():
                load_q(n + RING)

            @pl.when(n + RING == n_loads - 1)
            def _():
                load_q_last()

        take_relay(nk - 1)
        slot = (n_loads - 1) % RING
        for i in range(2):
            with jax.named_scope('wqh'):
                wait_half(slot, i)
            if i == 0:
                load_wo(1)
            r = slice(i * KC // 2, (i + 1) * KC // 2)
            acc[0:rows, :] += jnp.dot(xb[0:rows, d - KC + r.start:d - KC + r.stop], ring[slot, r, :],
                                      preferred_element_type=F32)

        def o_pair(i):
            first, count = ((0, groups - 1), (groups - 1, 1))[i]
            return remote(ob.at[pl.ds(0, rows), pl.ds(first * gw, count * gw)],
                          ob.at[pl.ds(0, rows), pl.ds(half + first * gw, count * gw)],
                          o_sem.at[2 * i], o_sem.at[2 * i + 1], partner)

        def attend(r0, r1, g, first, last, tri):
            n = r1 - r0
            cols = [slice(g * gw + m * HEAD, g * gw + (m + 1) * HEAD) for m in range(q_per)]
            q = jnp.concatenate([acc[r0:r1, c].astype(BF16) for c in cols], axis=0)
            s = lax.dot_general(q, kv[first:last, g * HEAD:(g + 1) * HEAD], (((1,), (1,)), ((), ())),
                                preferred_element_type=F32)
            lo, hi = tri - first, tri - first + n
            seen = lax.broadcasted_iota(jnp.int32, (n, n), 1) <= lax.broadcasted_iota(jnp.int32, (n, n), 0)
            seen = jnp.concatenate([jnp.where(seen, 1.0, 0.0)] * q_per, axis=0) > 0.5
            parts = [s[:, :lo]] * (lo > 0) + [jnp.where(seen, s[:, lo:hi], MASKED)] + [s[:, hi:]] * (hi < last - first)
            s = jnp.concatenate(parts, axis=1)
            top = jnp.max(s, axis=1, keepdims=True)
            e = jnp.exp2((s - top) * EXP_SCALE)
            w = (e * (1.0 / jnp.sum(e, axis=1, keepdims=True))).astype(BF16)
            o = jnp.dot(w, kv[first:last, kvw + g * HEAD:kvw + (g + 1) * HEAD], preferred_element_type=F32).astype(BF16)
            for m, c in enumerate(cols):
                ob[r0:r1, c] = o[m * n:(m + 1) * n, :]

        load_wo(2)
        mine = tabs.at[sp]
        for dev in (partner, across, diag):
            remote(mine, mine, t_sem.at[0], t_sem.at[1], dev).start()
        with jax.named_scope('wkvx'):
            kv_cross(kv_in).wait_recv()
        for g in range(groups):
            attend(0, own, g, 0, own if here == 0 else 2 * own, 0)
            attend(own, rows, g, 0 if here == 0 else own, rows, own)
            if g == groups - 2:
                with jax.named_scope('os'):
                    o_pair(0).start()
        with jax.named_scope('os'):
            o_pair(1).start()

        def h_cols(u, side=core):
            return pl.ds(pl.multiple_of(side * oh + units[u][0], HEAD), units[u][1])

        def h_pair(u):
            part = h_ref.at[pl.ds(0, rows), h_cols(u)]
            return remote(part, part, hp_sem.at[0], hp_sem.at[1], partner)

        def h_send(u):
            return remote(h_ref.at[pl.ds(given, own - given), h_cols(u)],
                          h_ref.at[pl.ds(own + given, own - given), h_cols(u)], hc_send, hc_recv.at[u], diag)

        def relay(u):
            part = h_ref.at[pl.ds(rows, own - red), h_cols(u, 1 - core)]
            with jax.named_scope('whc'):
                remote(part, part, hc_send, hc_recv.at[u], diag).wait_recv()
            remote(part, part, hr_sem.at[0], hr_sem.at[1], partner).start()

        def put(first, last, u, total):
            h_ref[first:last, h_cols(u)] = (xb[first:last, h_cols(u)].astype(F32) + total).astype(BF16)

        def finish(u, total):
            put(0, rows, u, total)
            h_send(u).start()
            h_pair(u).start()

        load_wo(3)
        for u in range(EARLY):
            wait_wo(u)
            oacc[u, 0:rows, :] = jnp.dot(ob[0:rows, 0:half], wob[u, 0:half, :], preferred_element_type=F32)
        load_wo(nu - 2)
        with jax.named_scope('wo'):
            o_pair(0).wait()
            o_pair(1).wait()
        for u in range(EARLY):
            finish(u, oacc[u, 0:rows, :] + jnp.dot(ob[0:rows, half:2 * half], wob[u, half:2 * half, :],
                                                   preferred_element_type=F32))
            if u == 0:
                load_wo(nu - 1)

        for u in range(EARLY, nu):
            if u < nu - 1:
                wait_wo(u)
                finish(u, times_wo(ob[0:rows, :], u))
            else:
                first, last = (0, rows) if here == 0 else (given, own)
                wait_half(units[u][2], 0)
                oacc[0, first:last, :] = times_wo(ob[first:last, 0:half], u, 0, half)
                with jax.named_scope('wwh'):
                    wait_half(units[u][2], 1)
                put(first, last, u, oacc[0, first:last, :] + times_wo(ob[first:last, half:2 * half], u, half, 2 * half))
                h_send(u).start()
                if here == 1:
                    o = jnp.concatenate([ob[0:given, :], ob[own:rows, :]], axis=0)
                    total = times_wo(o, u)
                    put(0, given, u, total[0:given])
                    put(own, rows, u, total[given:])
                h_pair(u).start()
            if u >= LAG:
                relay(u - LAG)
        build_picks()
        for u in range(nu - LAG, nu):
            relay(u)

        for k in range(2):
            if share(1 - here, k):
                @pl.when(core == k)
                def _():
                    n = share(1 - here, k)
                    part = xb.at[pl.ds(own + k * tok, n), :]
                    remote(x_ref.at[pl.ds(0, n), :], part, xc_send, xc_recv.at[0], across).wait_send()
            if share(here, k):
                @pl.when(core == k)
                def _():
                    part = xb.at[pl.ds(own + k * tok, share(here, k)), :]
                    remote(part, part, xr_send, xr_recv.at[0], partner).wait_send()
        kv_cross(kv_out).wait_send()

        with jax.named_scope('end'):
            sent = h_ref.at[pl.ds(given, own - given), pl.ds(0, oh)]
            shared = h_ref.at[pl.ds(0, rows), pl.ds(0, oh)]
            late = h_ref.at[pl.ds(rows, own - red), pl.ds(0, oh)]
            remote(sent, sent, hc_send, hc_recv.at[0], diag).wait_send()
            remote(shared, shared, hp_sem.at[0], hp_sem.at[1], partner).wait()
            remote(late, late, hr_sem.at[0], hr_sem.at[1], partner).wait()

    for c in range(2):
        pl.when(chip == c)(lambda: rest(c))


def dispatch_kernel(pick_ref, gate_ref, h_ref, hid_ref, buf_ref, out, sems):
    tok, d = hid_ref.shape
    held, tokens = buf_ref.shape[0], buf_ref.shape[1]
    core = lax.axis_index('sp') % 2
    own_rows = pl.ds(pl.multiple_of(core * tok, 16), tok)
    hidden = pltpu.make_async_copy(h_ref.at[own_rows, :], hid_ref, sems.at[0])
    hidden.start()
    for i in range(d // WIDE):
        c = slice(i * WIDE, (i + 1) * WIDE)
        y = jnp.dot(pick_ref[...], h_ref[:, c], preferred_element_type=F32)
        for e in range(held):
            r = slice(e * tokens, (e + 1) * tokens)
            g = gate_ref[r, :]
            for j in range(0, WIDE, HEAD):
                out[e, :, i * WIDE + j:i * WIDE + j + HEAD] = (g * y[r, j:j + HEAD]).astype(BF16)
        part = pl.ds(i * WIDE, WIDE)
        pltpu.make_async_copy(out.at[:, :, part], buf_ref.at[:, :, part], sems.at[1]).start()
    hidden.wait()
    pltpu.make_async_copy(out, buf_ref, sems.at[1]).wait()


def solution(mesh):
    row_spec = P(('dp', 'sp'), None)
    buf_spec = P(('dp', 'sp'), None, None)
    group = mesh.shape['sp']

    def device_step(x, w_q, w_k, w_v, w_o, ids, probs):
        tok, d = x.shape
        half, kvw, oh = w_q.shape[1] // 2, w_k.shape[1] // 2, d // 2
        experts = probs.shape[1]
        held = experts // group
        own, tokens = 2 * tok, group * tok
        rows = own + max(RED)
        nk, nn = d // KC, oh // NC
        any_spec = pl.BlockSpec(memory_space=pl.ANY)
        vmem_spec = pl.BlockSpec(memory_space=pltpu.VMEM)
        dma = pltpu.SemaphoreType.DMA
        h, pick, gate = pl.pallas_call(
            block_kernel,
            out_shape=(OUT_SPACE((tokens, d), BF16),
                       OUT_SPACE((held * tokens, tokens), BF16),
                       OUT_SPACE((held * tokens, 128), F32)),
            in_specs=[any_spec] * 7,
            out_specs=(vmem_spec,) * 3,
            scratch_shapes=[
                pltpu.VMEM((rows, d), BF16),
                pltpu.VMEM((RING, KC, half), BF16),
                pltpu.VMEM((WO_BUFS, d, NC), BF16),
                pltpu.VMEM((rows, half), F32),
                pltpu.VMEM((own, 2 * kvw), F32),
                pltpu.VMEM((tokens, 2 * kvw), BF16),
                pltpu.VMEM((rows, 2 * half), BF16),
                pltpu.VMEM((EARLY, rows, NC), F32),
                pltpu.VMEM((2, tok), jnp.int32),
                pltpu.VMEM((experts, tok), F32),
                pltpu.VMEM((group, 2 * experts, 128), F32),
                dma((RING,)), dma((2,)), dma((WO_BUFS,)), dma((3,)), dma((2,)),
                dma(()), dma((nk,)), dma(()), dma((nk,)),
                dma((2,)), dma((4,)), dma((2,)), dma(()), dma((nn,)), dma((2,)), dma((2,)),
            ],
            compiler_params=pltpu.CompilerParams(
                collective_id=0, has_side_effects=True, vmem_limit_bytes=BLOCK_VMEM),
            name='block',
        )(x, w_q, w_k, w_v, w_o, ids.T, probs.T)
        return pl.pallas_call(
            dispatch_kernel,
            out_shape=(jax.ShapeDtypeStruct((tok, d), BF16),
                       jax.ShapeDtypeStruct((held, tokens, d), BF16)),
            in_specs=[vmem_spec] * 3,
            out_specs=(any_spec,) * 2,
            scratch_shapes=[pltpu.VMEM((held, tokens, d), BF16), dma((2,))],
            compiler_params=pltpu.CompilerParams(vmem_limit_bytes=16_000_000),
            name='dispatch',
        )(pick, gate, h)

    return jax.shard_map(device_step, mesh=mesh,
                         in_specs=(row_spec, P(), P(), P(), P(), row_spec, row_spec),
                         out_specs=(row_spec, buf_spec), check_vma=False)
```

```python
import math
import jax
import jax.numpy as jnp
from jax import lax
from jax.experimental import pallas as pl
from jax.experimental.pallas import tpu as pltpu
from jax.sharding import PartitionSpec as P

MESH = pl.DeviceIdType.MESH
HEAD = 128
SCALE = 1.0 / math.sqrt(HEAD)
EXP_SCALE = math.log2(math.e) * SCALE
MASKED = -1e30 / SCALE
KC = 1024
NC = 512
RING = 3
WO_BUFS = 4
RED = (80, 64)
EARLY = 2
LAG = 4
FIRST = 2
KV_STEP = 3
WIDE = 512
BLOCK_VMEM = 59_000_000
OUT_SPACE = pltpu.VMEM
F32 = jnp.float32
BF16 = jnp.bfloat16


def block_kernel(x_ref, wq_ref, wk_ref, wv_ref, wo_ref, ids_ref, probs_ref,
                 h_ref, pick_ref, gate_ref,
                 xb, ring, wob, acc, kvacc, kv, ob, oacc, idsb, probsb, tabs,
                 ring_sem, half_sem, wo_sem, xp_sem, xc_send, xc_recv, xr_send, xr_recv,
                 kv_sem, o_sem, hp_sem, hc_send, hc_recv, t_sem):
    tok, d = x_ref.shape
    own = 2 * tok
    half = wq_ref.shape[1] // 2
    kvw = wk_ref.shape[1] // 2
    nk = d // KC
    per = half // (2 * kvw)
    n_kv = nk // per
    n_loads = n_kv + nk
    oh = d // 2
    nn = oh // NC
    groups = kvw // HEAD
    q_per = half // kvw
    gw = q_per * HEAD
    slots = [(n_loads - RING + i) % RING for i in range(2)]
    units = [(n * NC, NC, n) for n in range(WO_BUFS)]
    units += [((WO_BUFS + i) * NC, NC, slots[i]) for i in range(nn - WO_BUFS)]
    nu = len(units)

    sp = lax.axis_index('sp')
    chip = sp // 2
    core = sp % 2
    partner = chip * 2 + (1 - core)
    across = (1 - chip) * 2 + core
    diag = (1 - chip) * 2 + (1 - core)

    def remote(src, dst, send, recv, dev):
        return pltpu.make_async_remote_copy(
            src_ref=src, dst_ref=dst, send_sem=send, recv_sem=recv,
            device_id={'sp': dev}, device_id_type=MESH)

    def load_kv(n):
        for j in range(per):
            r = pl.ds((n * per + j) * KC, KC)
            c = pl.ds(pl.multiple_of(core * kvw, HEAD), kvw)
            pltpu.make_async_copy(wk_ref.at[r, c], ring.at[n, :, pl.ds(2 * j * kvw, kvw)], ring_sem.at[n]).start()
            pltpu.make_async_copy(wv_ref.at[r, c], ring.at[n, :, pl.ds((2 * j + 1) * kvw, kvw)], ring_sem.at[n]).start()

    def load_q(n):
        slot = n % RING
        r = pl.ds(pl.multiple_of((n - n_kv) * KC, KC), KC)
        c = pl.ds(pl.multiple_of(core * half, HEAD), half)
        pltpu.make_async_copy(wq_ref.at[r, c], ring.at[slot], ring_sem.at[slot]).start()

    def load_q_last():
        slot = (n_loads - 1) % RING
        c = pl.ds(pl.multiple_of(core * half, HEAD), half)
        for i in range(2):
            r = pl.ds(d - KC + i * KC // 2, KC // 2)
            pltpu.make_async_copy(wq_ref.at[r, c], ring.at[slot, pl.ds(i * KC // 2, KC // 2), :], half_sem.at[i]).start()

    def wait_half(slot, i):
        r = pl.ds(i * KC // 2, KC // 2)
        pltpu.make_async_copy(wq_ref.at[r, pl.ds(0, half)], ring.at[slot, r, :], half_sem.at[i]).wait()

    def wait_ring(slot):
        pltpu.make_async_copy(wq_ref.at[pl.ds(0, KC), pl.ds(0, half)], ring.at[slot], ring_sem.at[slot]).wait()

    def wo_part(u, j):
        width, slot = units[u][1:]
        return slot, pl.ds(j * width, width)

    def wo_sem_of(u):
        return wo_sem.at[u] if u < WO_BUFS else ring_sem.at[units[u][2]]

    def wo_copy_sem(u, j):
        return half_sem.at[j * KC // half] if u == nu - 1 else wo_sem_of(u)

    def load_wo(u):
        first, width, slot = units[u]
        c = pl.ds(pl.multiple_of(core * oh + first, HEAD), width)
        step = half if u < WO_BUFS else KC
        for j in range(2 * half // step):
            side = core if j * step < half else 1 - core
            r = pl.ds(pl.multiple_of(side * half + j * step % half, HEAD), step)
            if u < WO_BUFS:
                dst = wob.at[slot, pl.ds(j * step, step), :]
            else:
                dst = ring.at[slot, :, wo_part(u, j)[1]]
            pltpu.make_async_copy(wo_ref.at[r, c], dst, wo_copy_sem(u, j)).start()

    def wait_wo(u):
        width, slot = units[u][1:]
        if u < WO_BUFS:
            copy = pltpu.make_async_copy(wo_ref.at[:, pl.ds(0, NC)], wob.at[slot], wo_sem_of(u))
        else:
            n = half * width // NC
            copy = pltpu.make_async_copy(wq_ref.at[pl.ds(0, KC), pl.ds(0, n)], ring.at[slot, :, pl.ds(0, n)], wo_sem_of(u))
        with jax.named_scope('wwo'):
            copy.wait()

    def times_wo(o, u, first=0, last=2 * half):
        slot = units[u][2]
        if u < WO_BUFS:
            w = wob[slot, first:last, :]
        else:
            w = jnp.concatenate([ring[slot, :, wo_part(u, j)[1]] for j in range(first // KC, last // KC)], axis=0)
        return jnp.dot(o, w, preferred_element_type=F32)

    barrier = pltpu.get_barrier_semaphore()
    for dev in (partner, across, diag):
        pl.semaphore_signal(barrier, inc=1, device_id={'sp': dev}, device_id_type=MESH)

    own_rows = pl.ds(pl.multiple_of(core * tok, 16), tok)
    x_load = pltpu.make_async_copy(x_ref, xb.at[own_rows, :], wo_sem.at[0])
    ids_load = pltpu.make_async_copy(ids_ref, idsb, half_sem.at[0])
    probs_load = pltpu.make_async_copy(probs_ref, probsb, half_sem.at[1])
    x_load.start()
    ids_load.start()
    probs_load.start()
    load_kv(0)

    with jax.named_scope('bar'):
        pl.semaphore_wait(barrier, 3)

    x_pair = remote(x_ref, xb.at[own_rows, :], xp_sem.at[0], xp_sem.at[1], partner)
    x_pair.start()

    def share(c, k):
        return min(RED[c], tok) if k == 0 else max(RED[c] - tok, 0)

    def x_cross(c, k, j, early=False):
        n = share(c, k)
        cols = pl.ds(pl.multiple_of(j * KC, KC), KC)
        return remote(x_ref.at[pl.ds(0, n), cols] if early else xb.at[pl.ds(k * tok, n), cols], xb.at[pl.ds(own + k * tok, n), cols], xc_send, xc_recv.at[j], across)

    def x_relay(c, k, j):
        cols = pl.ds(pl.multiple_of(j * KC, KC), KC)
        part = xb.at[pl.ds(own + k * tok, share(c, k)), cols]
        return remote(part, part, xr_send, xr_recv.at[j], partner)

    for c in range(2):
        for k in range(2):
            if share(1 - c, k):
                @pl.when(jnp.logical_and(chip == c, core == k))
                def _():
                    for j in range(FIRST):
                        x_cross(1 - c, k, j, early=True).start()

    with jax.named_scope('xl'):
        x_load.wait()
    for c in range(2):
        @pl.when(jnp.logical_and(chip == c, core == 0))
        def _():
            for j in range(FIRST, nk):
                x_cross(1 - c, 0, j).start()
    for n in range(1, RING):
        if n < n_kv:
            load_kv(n)
        else:
            load_q(n)

    ids_load.wait()
    probs_load.wait()
    experts = probsb.shape[0]
    line = lax.broadcasted_iota(jnp.int32, (experts, tok), 0)
    pr = probsb[...]
    hit0 = line == idsb[0:1, :]
    hit1 = line == idsb[1:2, :]
    p0 = jnp.sum(jnp.where(hit0, pr, 0.0), axis=0, keepdims=True)
    p1 = jnp.sum(jnp.where(hit1, pr, 0.0), axis=0, keepdims=True)
    hit = jnp.logical_or(hit0, hit1)
    tabs[sp] = jnp.zeros(tabs.shape[1:], F32)
    tabs[sp, 0:experts, 0:tok] = jnp.where(hit, pr / (p0 + p1), 0.0)
    tabs[sp, experts:2 * experts, 0:tok] = jnp.where(hit, 1.0, 0.0)
    acc[...] = jnp.zeros_like(acc)
    kvacc[...] = jnp.zeros_like(kvacc)

    with jax.named_scope('wxp'):
        x_pair.wait()

    @pl.loop(0, n_kv)
    def _(n):
        with jax.named_scope('wkv'):
            wait_ring(n)
        for j in range(per):
            c = pl.ds(pl.multiple_of((n * per + j) * KC, KC), KC)
            kvacc[...] += jnp.dot(xb[0:own, c], ring[n, :, 2 * j * kvw:2 * (j + 1) * kvw],
                                  preferred_element_type=F32)
        load_q(n + RING)

    for c in range(2):
        if share(1 - c, 1):
            @pl.when(jnp.logical_and(chip == c, core == 1))
            def _():
                for j in range(FIRST, nk):
                    x_cross(1 - c, 1, j).start()

    kv[0:own, :] = kvacc[...].astype(BF16)

    def build_picks():
        with jax.named_scope('tab'):
            three = tabs.at[pl.ds(0, 3)]
            remote(three, three, t_sem.at[0], t_sem.at[1], partner).wait()
        lanes = tabs.shape[2]
        tokens = pick_ref.shape[1]
        held = pick_ref.shape[0] // tokens
        before = lax.broadcasted_iota(jnp.int32, (lanes, lanes), 0) < lax.broadcasted_iota(jnp.int32, (lanes, lanes), 1)
        before = jnp.where(before, 1.0, 0.0).astype(BF16)
        dests, gates = [], []
        for j in range(2):
            dest, g = 0.0, 0.0
            for i in range(2):
                s = (chip if j == 0 else 1 - chip) * 2 + i
                hits = tabs[s, experts:2 * experts, :]
                rank = jnp.dot(hits.astype(BF16), before, preferred_element_type=F32)
                at = jnp.where(hits > 0.5, rank + (s * tok + 1).astype(F32), 0.0)
                gs = tabs[s, 0:experts, :]
                dest = dest + (at if i == 0 else pltpu.roll(at, tok, 1))
                g = g + (gs if i == 0 else pltpu.roll(gs, tok, 1))
            dests.append(dest)
            gates.append(g)
        line = lax.broadcasted_iota(jnp.int32, (experts, lanes), 0)
        slot = lax.broadcasted_iota(jnp.int32, (tokens, lanes), 0).astype(F32) + 1.0
        for e in range(held):
            total = jnp.zeros((tokens, 1), F32)
            for j in range(2):
                here = line == sp * held + e
                dest = jnp.sum(jnp.where(here, dests[j], 0.0), axis=0, keepdims=True)
                g = jnp.sum(jnp.where(here, gates[j], 0.0), axis=0, keepdims=True)
                chosen = slot == dest
                pick_ref[e * tokens:(e + 1) * tokens, j * lanes:(j + 1) * lanes] = jnp.where(chosen, 1.0, 0.0).astype(BF16)
                total = total + jnp.sum(jnp.where(chosen, g, 0.0), axis=1, keepdims=True)
            gate_ref[e * tokens:(e + 1) * tokens, :] = jnp.broadcast_to(total, (tokens, lanes))

    def rest(here):
        red = RED[here]
        rows = own + red
        given = RED[1 - here]
        kv_out, kv_in = (own, red) if here == 0 else (given, own)

        def kv_cross(count):
            return remote(kv.at[pl.ds(0, count), :], kv.at[pl.ds(own, count), :], kv_sem.at[0], kv_sem.at[1], across)

        def pass_on(j):
            for k in range(2):
                if share(here, k):
                    @pl.when(core == k)
                    def _():
                        with jax.named_scope('wxc'):
                            x_cross(here, k, j).wait_recv()
                        x_relay(here, k, j).start()

        @pl.when(core == 0)
        def _():
            kv_cross(kv_out).start()

        pass_on(0)

        def take_relay(j):
            for k in range(2):
                if share(here, k):
                    @pl.when(core == 1 - k)
                    def _():
                        with jax.named_scope('wxr'):
                            x_relay(here, k, j).wait_recv()

        @pl.loop(0, nk - 1)
        def _(j):
            pass_on(j + 1)
            take_relay(j)

            @pl.when(jnp.logical_and(core == 1, j == KV_STEP))
            def _():
                kv_cross(kv_out).start()

            n = n_kv + j
            slot = n % RING
            with jax.named_scope('wq'):
                wait_ring(slot)

            @pl.when(j == nk - 2)
            def _():
                load_wo(0)

            c = pl.ds(pl.multiple_of(j * KC, KC), KC)
            acc[0:rows, :] += jnp.dot(xb[0:rows, c], ring[slot], preferred_element_type=F32)

            @pl.when(n + RING < n_loads - 1)
            def _():
                load_q(n + RING)

            @pl.when(n + RING == n_loads - 1)
            def _():
                load_q_last()

        take_relay(nk - 1)
        slot = (n_loads - 1) % RING
        for i in range(2):
            with jax.named_scope('wqh'):
                wait_half(slot, i)
            if i == 0:
                load_wo(1)
            r = slice(i * KC // 2, (i + 1) * KC // 2)
            acc[0:rows, :] += jnp.dot(xb[0:rows, d - KC + r.start:d - KC + r.stop], ring[slot, r, :],
                                      preferred_element_type=F32)

        def o_pair(i):
            first, count = ((0, groups - 1), (groups - 1, 1))[i]
            return remote(ob.at[pl.ds(0, rows), pl.ds(first * gw, count * gw)],
                          ob.at[pl.ds(0, rows), pl.ds(half + first * gw, count * gw)],
                          o_sem.at[2 * i], o_sem.at[2 * i + 1], partner)

        def attend(r0, r1, g, first, last, tri):
            n = r1 - r0
            cols = [slice(g * gw + m * HEAD, g * gw + (m + 1) * HEAD) for m in range(q_per)]
            q = jnp.concatenate([acc[r0:r1, c].astype(BF16) for c in cols], axis=0)
            s = lax.dot_general(q, kv[first:last, g * HEAD:(g + 1) * HEAD], (((1,), (1,)), ((), ())),
                                preferred_element_type=F32)
            lo, hi = tri - first, tri - first + n
            seen = lax.broadcasted_iota(jnp.int32, (n, n), 1) <= lax.broadcasted_iota(jnp.int32, (n, n), 0)
            seen = jnp.concatenate([jnp.where(seen, 1.0, 0.0)] * q_per, axis=0) > 0.5
            parts = [s[:, :lo]] * (lo > 0) + [jnp.where(seen, s[:, lo:hi], MASKED)] + [s[:, hi:]] * (hi < last - first)
            s = jnp.concatenate(parts, axis=1)
            top = jnp.max(s, axis=1, keepdims=True)
            e = jnp.exp2((s - top) * EXP_SCALE)
            w = (e * (1.0 / jnp.sum(e, axis=1, keepdims=True))).astype(BF16)
            o = jnp.dot(w, kv[first:last, kvw + g * HEAD:kvw + (g + 1) * HEAD], preferred_element_type=F32).astype(BF16)
            for m, c in enumerate(cols):
                ob[r0:r1, c] = o[m * n:(m + 1) * n, :]

        load_wo(2)
        mine = tabs.at[sp]
        for dev in (partner, across, diag):
            remote(mine, mine, t_sem.at[0], t_sem.at[1], dev).start()
        with jax.named_scope('wkvx'):
            kv_cross(kv_in).wait_recv()
        for g in range(groups):
            attend(0, own, g, 0, own if here == 0 else 2 * own, 0)
            attend(own, rows, g, 0 if here == 0 else own, rows, own)
            if g == groups - 2:
                with jax.named_scope('os'):
                    o_pair(0).start()
        with jax.named_scope('os'):
            o_pair(1).start()

        def h_cols(u, side=core):
            return pl.ds(pl.multiple_of(side * oh + units[u][0], HEAD), units[u][1])

        def h_pair(u):
            part = h_ref.at[pl.ds(0, rows), h_cols(u)]
            return remote(part, part, hp_sem.at[0], hp_sem.at[1], partner)

        def h_send(u):
            return remote(h_ref.at[pl.ds(given, own - given), h_cols(u)],
                          h_ref.at[pl.ds(own + given, own - given), h_cols(u)], hc_send, hc_recv.at[u], diag)

        def relay(u):
            part = h_ref.at[pl.ds(rows, own - red), h_cols(u, 1 - core)]
            with jax.named_scope('whc'):
                remote(part, part, hc_send, hc_recv.at[u], diag).wait_recv()
            remote(part, part, hp_sem.at[0], hp_sem.at[1], partner).start()

        def put(first, last, u, total):
            h_ref[first:last, h_cols(u)] = (xb[first:last, h_cols(u)].astype(F32) + total).astype(BF16)

        def finish(u, total):
            put(0, rows, u, total)
            h_send(u).start()
            h_pair(u).start()

        load_wo(3)
        for u in range(EARLY):
            wait_wo(u)
            oacc[u, 0:rows, :] = jnp.dot(ob[0:rows, 0:half], wob[u, 0:half, :], preferred_element_type=F32)
        load_wo(nu - 2)
        with jax.named_scope('wo'):
            o_pair(0).wait()
            o_pair(1).wait()
        for u in range(EARLY):
            finish(u, oacc[u, 0:rows, :] + jnp.dot(ob[0:rows, half:2 * half], wob[u, half:2 * half, :],
                                                   preferred_element_type=F32))
            if u == 0:
                load_wo(nu - 1)

        for u in range(EARLY, nu):
            if u < nu - 1:
                wait_wo(u)
                finish(u, times_wo(ob[0:rows, :], u))
            else:
                first, last = (0, rows) if here == 0 else (given, own)
                wait_half(units[u][2], 0)
                oacc[0, first:last, :] = times_wo(ob[first:last, 0:half], u, 0, half)
                with jax.named_scope('wwh'):
                    wait_half(units[u][2], 1)
                put(first, last, u, oacc[0, first:last, :] + times_wo(ob[first:last, half:2 * half], u, half, 2 * half))
                h_send(u).start()
                if here == 1:
                    o = jnp.concatenate([ob[0:given, :], ob[own:rows, :]], axis=0)
                    total = times_wo(o, u)
                    put(0, given, u, total[0:given])
                    put(own, rows, u, total[given:])
                h_pair(u).start()
            if u >= LAG:
                relay(u - LAG)
        build_picks()
        for u in range(nu - LAG, nu):
            relay(u)

        for k in range(2):
            if share(1 - here, k):
                @pl.when(core == k)
                def _():
                    n = share(1 - here, k)
                    part = xb.at[pl.ds(own + k * tok, n), :]
                    remote(x_ref.at[pl.ds(0, n), :], part, xc_send, xc_recv.at[0], across).wait_send()
            if share(here, k):
                @pl.when(core == k)
                def _():
                    part = xb.at[pl.ds(own + k * tok, share(here, k)), :]
                    remote(part, part, xr_send, xr_recv.at[0], partner).wait_send()
        kv_cross(kv_out).wait_send()

        with jax.named_scope('end'):
            sent = h_ref.at[pl.ds(given, own - given), pl.ds(0, oh)]
            whole = h_ref.at[:, pl.ds(0, oh)]
            remote(sent, sent, hc_send, hc_recv.at[0], diag).wait_send()
            remote(whole, whole, hp_sem.at[0], hp_sem.at[1], partner).wait()

    for c in range(2):
        pl.when(chip == c)(lambda: rest(c))


def dispatch_kernel(pick_ref, gate_ref, h_ref, hid_ref, buf_ref, out, sems):
    tok, d = hid_ref.shape
    held, tokens = buf_ref.shape[0], buf_ref.shape[1]
    core = lax.axis_index('sp') % 2
    own_rows = pl.ds(pl.multiple_of(core * tok, 16), tok)
    hidden = pltpu.make_async_copy(h_ref.at[own_rows, :], hid_ref, sems.at[0])
    hidden.start()
    for i in range(d // WIDE):
        c = slice(i * WIDE, (i + 1) * WIDE)
        y = jnp.dot(pick_ref[...], h_ref[:, c], preferred_element_type=F32)
        for e in range(held):
            r = slice(e * tokens, (e + 1) * tokens)
            g = gate_ref[r, :]
            for j in range(0, WIDE, HEAD):
                out[e, :, i * WIDE + j:i * WIDE + j + HEAD] = (g * y[r, j:j + HEAD]).astype(BF16)
        part = pl.ds(i * WIDE, WIDE)
        pltpu.make_async_copy(out.at[:, :, part], buf_ref.at[:, :, part], sems.at[1]).start()
    hidden.wait()
    pltpu.make_async_copy(out, buf_ref, sems.at[1]).wait()


def solution(mesh):
    row_spec = P(('dp', 'sp'), None)
    buf_spec = P(('dp', 'sp'), None, None)
    group = mesh.shape['sp']

    def device_step(x, w_q, w_k, w_v, w_o, ids, probs):
        tok, d = x.shape
        half, kvw, oh = w_q.shape[1] // 2, w_k.shape[1] // 2, d // 2
        experts = probs.shape[1]
        held = experts // group
        own, tokens = 2 * tok, group * tok
        rows = own + max(RED)
        nk, nn = d // KC, oh // NC
        any_spec = pl.BlockSpec(memory_space=pl.ANY)
        vmem_spec = pl.BlockSpec(memory_space=pltpu.VMEM)
        dma = pltpu.SemaphoreType.DMA
        h, pick, gate = pl.pallas_call(
            block_kernel,
            out_shape=(OUT_SPACE((tokens, d), BF16),
                       OUT_SPACE((held * tokens, tokens), BF16),
                       OUT_SPACE((held * tokens, 128), F32)),
            in_specs=[any_spec] * 7,
            out_specs=(vmem_spec,) * 3,
            scratch_shapes=[
                pltpu.VMEM((rows, d), BF16),
                pltpu.VMEM((RING, KC, half), BF16),
                pltpu.VMEM((WO_BUFS, d, NC), BF16),
                pltpu.VMEM((rows, half), F32),
                pltpu.VMEM((own, 2 * kvw), F32),
                pltpu.VMEM((tokens, 2 * kvw), BF16),
                pltpu.VMEM((rows, 2 * half), BF16),
                pltpu.VMEM((EARLY, rows, NC), F32),
                pltpu.VMEM((2, tok), jnp.int32),
                pltpu.VMEM((experts, tok), F32),
                pltpu.VMEM((group, 2 * experts, 128), F32),
                dma((RING,)), dma((2,)), dma((WO_BUFS,)), dma((2,)),
                dma(()), dma((nk,)), dma(()), dma((nk,)),
                dma((2,)), dma((4,)), dma((2,)), dma(()), dma((nn,)), dma((2,)),
            ],
            compiler_params=pltpu.CompilerParams(
                collective_id=0, has_side_effects=True, vmem_limit_bytes=BLOCK_VMEM),
            name='block',
        )(x, w_q, w_k, w_v, w_o, ids.T, probs.T)
        return pl.pallas_call(
            dispatch_kernel,
            out_shape=(jax.ShapeDtypeStruct((tok, d), BF16),
                       jax.ShapeDtypeStruct((held, tokens, d), BF16)),
            in_specs=[vmem_spec] * 3,
            out_specs=(any_spec,) * 2,
            scratch_shapes=[pltpu.VMEM((held, tokens, d), BF16), dma((2,))],
            compiler_params=pltpu.CompilerParams(vmem_limit_bytes=16_000_000),
            name='dispatch',
        )(pick, gate, h)

    return jax.shard_map(device_step, mesh=mesh,
                         in_specs=(row_spec, P(), P(), P(), P(), row_spec, row_spec),
                         out_specs=(row_spec, buf_spec), check_vma=False)
```
